128 devices in a mesh: lat: 32 (over y, z, core), fld: 4 (over x).
Axes of the slice: x: 4, y: 4, z: 4, core: 2. Of those that a mesh axis runs over, the one named last changes fastest.
Arguments:
- grid_fields: bfloat16 [96, 1280, 2560], P('fld', 'lat'), may hold values from -6 to 6
- assign: int32 [320], replicated, may hold values from 0 to 319, each once
- limits: int32 [3], replicated, may hold values from 60 to 319, as said below
- legendre: bfloat16 [320, 641, 640], P('lat', None, 'fld'), may hold values from -0.25 to 0.25
- synth_one: bfloat16 [320, 320, 320], P('lat'), may hold values from -0.3125 to 0.3125
- synth_two: bfloat16 [320, 160, 160], P('lat'), may hold values from -0.5 to 0.5
- synth_three: bfloat16 [320, 80, 80], P('lat'), may hold values from -0.625 to 0.625
Outputs:
- spectrum: bfloat16 [96, 2, 320, 641], P('fld', None, 'lat')
- grid_one: float32 [96, 640, 1280], P('fld', 'lat')
- grid_two: float32 [96, 320, 640], P('fld', 'lat')
- grid_three: float32 [96, 160, 320], P('fld', 'lat')
The draws below stay inside these ranges and needn't reach their ends.
Inputs may be any that keep to these rules, and one draw needn't show every extreme that they name: assign is a permutation; slot q stands for the wavenumbers assign[q] and 639 - assign[q]. limits[0] is 319, limits[2] is 60, and limits[1] lies between 120 and 159.
All inputs are finite; a program needn't handle non-finite values.
Results may differ from the reference program's by a relative error of at most 0.0077.
Values may be sent and summed in bfloat16 or wider, within the bound.
A program may use at most 128 MiB of HBM per device.

```python
import math
import jax
import jax.numpy as jnp

MW = 640
NLAT = 1280
NLON = 2560
FIELDS = 96
PAIRS = 320
PACK = 641
NH = 640
MW1 = 320
MW2 = 160
MW3 = 80


def draw_limits(key, part):
    counts = jnp.array([MW // 2, MW // 4, MW // 8], dtype=jnp.int32)
    middle = jax.random.randint(key, (), 0, MW // 4 // 4, dtype=jnp.int32)
    offsets = jnp.stack([jnp.zeros((), jnp.int32), middle, jnp.full((), MW // 8 // 4, jnp.int32)])
    return counts - 1 - offsets + jnp.array([0, 0, 1], dtype=jnp.int32)


def level_of(own_key, extent, pieces, least, top_value):
    factor_of = 1.0
    for axis_at, parts in pieces:
        steps = jax.random.uniform(jax.random.fold_in(jax.random.fold_in(own_key, 6), axis_at), (parts,), jnp.float32, least / len(pieces), top_value / len(pieces))
        factor_of = factor_of * jnp.repeat(jnp.exp(steps), extent[axis_at] // parts).reshape((-1,) + (1,) * (len(extent) - 1 - axis_at))
    return factor_of


def centred(rng, shape, spread, reach, pieces=(), kind=jnp.bfloat16):
    values = spread * jax.random.normal(rng, shape, jnp.float32)
    if pieces:
        values = values * level_of(rng, shape, pieces, -0.22, 0.18)
    return jnp.clip(values, -reach, reach).astype(kind)


def setup_inputs(seed: int = 0) -> dict:
    splits = jax.random.split(jax.random.key(seed), 8)
    grid_fields = centred(splits[0], (FIELDS, NLAT, NLON), 1.0, 6.0, ((0, 4), (1, 32)))
    assign = jax.random.permutation(splits[1], PAIRS).astype(jnp.int32)
    limits = draw_limits(jax.random.fold_in(splits[7], 71), 0)
    legendre = centred(splits[3], (PAIRS, PACK, NH), NH ** -0.5, 0.25, ((0, 32), (2, 4)))
    synth_one = centred(splits[4], (PAIRS, MW1, MW1), MW1 ** -0.5, 0.3125, ((0, 32),))
    synth_two = centred(splits[5], (PAIRS, MW2, MW2), MW2 ** -0.5, 0.5, ((0, 32),))
    synth_three = centred(splits[6], (PAIRS, MW3, MW3), MW3 ** -0.5, 0.625, ((0, 32),))
    return dict(grid_fields=grid_fields, assign=assign, limits=limits, legendre=legendre, synth_one=synth_one, synth_two=synth_two, synth_three=synth_three)


def phases(lon_length, wavenums):
    places = jnp.arange(lon_length, dtype=jnp.int32)
    turn_count = places[:, None] * wavenums[None, :].astype(jnp.int32) % lon_length
    angle = turn_count.astype(jnp.float32) * (2.0 * math.pi / lon_length)
    return (jnp.cos(angle), jnp.sin(angle))

def choose_pair(values, limit_of):
    ranks = jnp.arange(values.shape[-1], dtype=jnp.int32)
    keep_mask = ranks[None, :] < limit_of[:, None]
    return jnp.where(keep_mask[None, None], values[:, :, :, 0], values[:, :, :, 1])

def select_rows(sym_prod, anti_prod, own_pairs, wave_total):
    first_rows = choose_pair(sym_prod, (wave_total + 1 - own_pairs) // 2)
    later_rows = choose_pair(anti_prod, (wave_total - own_pairs) // 2)
    return jnp.concatenate([first_rows, later_rows], axis=3)

def level_field(spectrum, own_pairs, limit, synth_table):
    half_rows = synth_table.shape[1] // 2
    sym_rows = spectrum.shape[3] // 2 + 1
    step_rows = 2 * jnp.arange(half_rows, dtype=jnp.int32)
    keep_sym = own_pairs[:, None] + step_rows[None, :] <= limit
    keep_anti = own_pairs[:, None] + 1 + step_rows[None, :] <= limit
    zero_value = jnp.zeros((), jnp.bfloat16)
    kept_sym = jnp.where(keep_sym[None, None], spectrum[..., :half_rows], zero_value)
    kept_anti = jnp.where(keep_anti[None, None], spectrum[..., sym_rows:sym_rows + half_rows], zero_value)
    even_part = jnp.einsum('fcqk,qkj->fcjq', kept_sym.astype(jnp.float32), synth_table[:, :half_rows].astype(jnp.float32))
    odd_part = jnp.einsum('fcqk,qkj->fcjq', kept_anti.astype(jnp.float32), synth_table[:, half_rows:].astype(jnp.float32))
    return jnp.concatenate([even_part + odd_part, jnp.flip(even_part - odd_part, axis=2)], axis=2).astype(jnp.bfloat16)

def inverse_table(assign, lon_length):
    cosine, sine_part = phases(lon_length, assign)
    weight = jnp.where(assign == 0, 1.0, 2.0).astype(jnp.float32) / math.sqrt(lon_length)
    return jnp.stack([cosine.T * weight[:, None], -sine_part.T * weight[:, None]], axis=0).astype(jnp.bfloat16)

def reference(grid_fields, assign, limits, legendre, synth_one, synth_two, synth_three):
    pair_total = assign.shape[0]
    wave_total = 2 * pair_total
    sym_rows = pair_total + 1
    field_count, lat_total, lon_total = grid_fields.shape
    half_lat = lat_total // 2
    wavenums = jnp.stack([assign, wave_total - 1 - assign], axis=1).reshape(-1)
    cosine, sine_part = phases(lon_total, wavenums)
    dft_scale = 1.0 / math.sqrt(lon_total)
    dft_table = jnp.stack([cosine * dft_scale, -sine_part * dft_scale], axis=1).reshape(lon_total, -1).astype(jnp.bfloat16)
    fourier = jnp.dot(grid_fields.reshape(-1, lon_total), dft_table, preferred_element_type=jnp.float32).astype(jnp.bfloat16)
    split_four = fourier.reshape(field_count, lat_total, 2, pair_total, 2).astype(jnp.float32)
    north_rows = split_four[:, :half_lat]
    south_rows = jnp.flip(split_four[:, half_lat:], axis=1)
    symmetric = (north_rows + south_rows).astype(jnp.bfloat16)
    antisym = (north_rows - south_rows).astype(jnp.bfloat16)
    sym_prod = jnp.einsum('kjcsw,srj->kcswr', symmetric.astype(jnp.float32), legendre[:, :sym_rows].astype(jnp.float32))
    anti_prod = jnp.einsum('kjcsw,srj->kcswr', antisym.astype(jnp.float32), legendre[:, sym_rows:].astype(jnp.float32))
    spectrum = select_rows(sym_prod, anti_prod, assign, wave_total).astype(jnp.bfloat16)
    grids_out = []
    for level_index, synth_table in enumerate((synth_one, synth_two, synth_three)):
        level_rows = level_field(spectrum, assign, limits[level_index], synth_table)
        inverse = inverse_table(assign, 4 * synth_table.shape[1])
        grids_out.append(jnp.einsum('fcjq,cqi->fji', level_rows.astype(jnp.float32), inverse.astype(jnp.float32)))
    return (spectrum, grids_out[0], grids_out[1], grids_out[2])
```

```python
import math

import jax
import jax.numpy as jnp
from jax import lax
from jax.experimental import pallas as pl
from jax.experimental.pallas import tpu as pltpu
from jax.sharding import PartitionSpec as P

MESH = pl.DeviceIdType.MESH
F32 = jnp.float32
BF16 = jnp.bfloat16
NLAT = 32
NFLD = 4
FLD = 24
ROWS = 40
LON = 2560
PAIR = 10
SENT = (20, 10, 5)
LEVELS = (320, 160, 80)
NT = (((1,), (1,)), ((), ()))


def sincos(turns):
    quarter = jnp.floor(turns * 4.0 + 0.5)
    y = (turns * 4.0 - quarter) * (math.pi / 2)
    y2 = y * y
    s = y * (1.0 + y2 * (-1.0 / 6 + y2 * (1.0 / 120 - y2 * (1.0 / 5040))))
    c = 1.0 + y2 * (-0.5 + y2 * (1.0 / 24 + y2 * (-1.0 / 720 + y2 * (1.0 / 40320))))
    k = quarter - 4.0 * jnp.floor(quarter * 0.25)
    odd = (k == 1.0) | (k == 3.0)
    sin_v = jnp.where(odd, c, s)
    cos_v = jnp.where(odd, s, c)
    sin_v = jnp.where(k >= 2.0, -sin_v, sin_v)
    cos_v = jnp.where((k == 1.0) | (k == 2.0), -cos_v, cos_v)
    return cos_v, sin_v


def turns_of(product, period):
    return (product - period * jnp.floor(product * (1.0 / period))) * (1.0 / period)


def fill_table(cols_ref, first, count, period, scale, tiles, store):
    wave = jnp.broadcast_to(cols_ref[pl.ds(first, count), 0:1], (count, 128))
    amp = jnp.broadcast_to(cols_ref[pl.ds(first, count), 1:2], (count, 128)) * scale
    comp = jnp.broadcast_to(cols_ref[pl.ds(first, count), 2:3], (count, 128))
    lane = lax.broadcasted_iota(jnp.int32, (count, 128), 1).astype(F32)
    cos_v, sin_v = sincos(turns_of(wave * lane + comp * (period // 4), float(period)))
    cos_d, sin_d = sincos(turns_of(wave * 128.0, float(period)))
    cos_v, sin_v = cos_v * amp, sin_v * amp
    for a in range(tiles):
        store(a, cos_v)
        if a + 1 < tiles:
            cos_v, sin_v = cos_v * cos_d - sin_v * sin_d, sin_v * cos_d + cos_v * sin_d


def pack_kernel(where_ref, a_ref, main_ref, extra_ref):
    q = pl.program_id(0)
    a = a_ref[0].astype(F32)
    t = [a[:, 128 * k : 128 * k + 128] for k in range(5)]
    last = a[:, 640:641]
    lane = lax.broadcasted_iota(jnp.int32, (a.shape[0], 128), 1)
    r = [None, None] + [pltpu.roll(t[k], 63, 1) for k in (2, 3, 4)]
    main_ref[0, :, 0:128] = t[0].astype(BF16)
    main_ref[0, :, 128:256] = t[1].astype(BF16)
    main_ref[0, :, 256:384] = jnp.where(lane < 63, r[2], r[3]).astype(BF16)
    main_ref[0, :, 384:512] = jnp.where(lane < 63, r[3], r[4]).astype(BF16)
    tail = jnp.where(lane < 127, pltpu.roll(t[4], 127, 1), last)
    main_ref[0, :, 512:640] = jnp.where(lane < 64, t[2], tail).astype(BF16)
    column = jnp.sum(jnp.where(lane == 64, t[2], 0.0), axis=1, keepdims=True)

    @pl.when(q == 0)
    def _():
        extra_ref[...] = jnp.zeros_like(extra_ref)

    extra_ref[...] = jnp.where(lane == q, column, extra_ref[...].astype(F32)).astype(BF16)


def pack(legendre_t, fld):
    rows = legendre_t.shape[1]
    return pl.pallas_call(
        pack_kernel,
        grid_spec=pltpu.PrefetchScalarGridSpec(
            num_scalar_prefetch=1,
            grid=(PAIR,),
            in_specs=[pl.BlockSpec((1, rows, 641), lambda q, w: (q, 0, 0))],
            out_specs=[
                pl.BlockSpec((1, rows, 640), lambda q, w: (q, w[0], 0)),
                pl.BlockSpec((rows, 128), lambda q, w: (w[0], 0)),
            ],
        ),
        out_shape=[
            jax.ShapeDtypeStruct((PAIR, NFLD * rows, 640), BF16),
            jax.ShapeDtypeStruct((NFLD * rows, 128), BF16),
        ],
    )(fld, legendre_t)


def dft_kernel(cols_ref, perm_ref, g_ref, out_ref, table, folded):
    step = pl.program_id(0)

    @pl.when(step == 0)
    def _():
        folded[...] = jnp.zeros_like(folded)

        def block(b, carry):
            first = pl.multiple_of(b * 64, 64)

            def store(a, value):
                table[pl.ds(first, 64), 128 * a : 128 * a + 128] = value.astype(BF16)

            fill_table(cols_ref, first, 64, LON, 1.0 / math.sqrt(LON), 10, store)
            return carry

        lax.fori_loop(0, 24, block, 0)

    g = g_ref[...].astype(F32)
    low = g[:, :, : LON // 2].reshape(240, LON // 2)
    high = g[:, :, LON // 2 :].reshape(240, LON // 2)
    for par in range(2):
        x = low + high if par == 0 else low - high
        folded[0:120] = x[0:120].astype(BF16)
        folded[128:248] = x[120:240].astype(BF16)
        y = lax.dot_general(
            table[768 * par : 768 * par + 768], folded[...], NT, preferred_element_type=F32
        )
        y = jnp.dot(y.astype(BF16), perm_ref[...], preferred_element_type=F32)
        out_ref[:, par] = y.reshape(NLAT, 24, 256).astype(BF16)


def dft(cols, perm, grid_fields):
    return pl.pallas_call(
        dft_kernel,
        grid=(4,),
        in_specs=[
            pl.BlockSpec((1536, 8), lambda g: (0, 0)),
            pl.BlockSpec((256, 256), lambda g: (0, 0)),
            pl.BlockSpec((6, ROWS, LON), lambda g: (g, 0, 0)),
        ],
        out_specs=pl.BlockSpec((NLAT, 2, 24, 256), lambda g: (0, 0, 0, g)),
        out_shape=jax.ShapeDtypeStruct((NLAT, 2, 24, 1024), BF16),
        scratch_shapes=[
            pltpu.VMEM((1536, LON // 2), BF16),
            pltpu.VMEM((256, LON // 2), BF16),
        ],
    )(cols, perm, grid_fields)


def lat_peer(k):
    return lax.rem(lax.axis_index("lat") + k, NLAT)


def greet(barrier, with_fld):
    fld = lax.axis_index("fld")
    lat = lax.axis_index("lat")

    def one(k, carry):
        pl.semaphore_signal(barrier, inc=1, device_id=(lat_peer(k), fld), device_id_type=MESH)
        return carry

    lax.fori_loop(1, NLAT, one, 0)
    count = NLAT - 1
    if with_fld:
        for k in range(1, NFLD):
            pl.semaphore_signal(
                barrier, inc=1, device_id=(lat, lax.rem(fld + k, NFLD)), device_id_type=MESH
            )
        count += NFLD - 1
    pl.semaphore_wait(barrier, count)


def exchange_copy(src, dst, send_sem, recv_sem, k):
    return pltpu.make_async_remote_copy(
        src_ref=src.at[lat_peer(k)],
        dst_ref=dst.at[lax.axis_index("lat")],
        send_sem=send_sem.at[k - 1],
        recv_sem=recv_sem.at[k - 1],
        device_id=(lat_peer(k), lax.axis_index("fld")),
        device_id_type=MESH,
    )


def start_exchange(src, dst, send_sem, recv_sem, own_sem):
    lat = lax.axis_index("lat")
    pltpu.make_async_copy(src.at[lat], dst.at[lat], own_sem).start()

    def one(k, carry):
        exchange_copy(src, dst, send_sem, recv_sem, k).start()
        return carry

    lax.fori_loop(1, NLAT, one, 0)


def end_exchange(src, dst, send_sem, recv_sem, own_sem):
    lat = lax.axis_index("lat")

    def one(k, carry):
        exchange_copy(src, dst, send_sem, recv_sem, k).wait()
        return carry

    lax.fori_loop(1, NLAT, one, 0)
    pltpu.make_async_copy(src.at[lat], dst.at[lat], own_sem).wait()


def exchange_kernel(src, dst, send_sem, recv_sem, own_sem):
    greet(pltpu.get_barrier_semaphore(), False)
    start_exchange(src, dst, send_sem, recv_sem, own_sem)
    end_exchange(src, dst, send_sem, recv_sem, own_sem)


def exchange(blocks):
    return pl.pallas_call(
        exchange_kernel,
        in_specs=[pl.BlockSpec(memory_space=pltpu.HBM)],
        out_specs=pl.BlockSpec(memory_space=pltpu.HBM),
        out_shape=jax.ShapeDtypeStruct(blocks.shape, blocks.dtype),
        scratch_shapes=[
            pltpu.SemaphoreType.DMA((NLAT - 1,)),
            pltpu.SemaphoreType.DMA((NLAT - 1,)),
            pltpu.SemaphoreType.DMA,
        ],
        compiler_params=pltpu.CompilerParams(collective_id=1, has_side_effects=True),
    )(blocks)


def move_kernel(
    y, main_in, extra_in, x, main, extra, send_sem, recv_sem, own_sem, ring_send, ring_recv,
    relay_send, relay_recv, extra_send, extra_recv,
):
    lat = lax.axis_index("lat")
    fld = lax.axis_index("fld")
    rows = main.shape[1] // NFLD
    greet(pltpu.get_barrier_semaphore(), True)

    def shard(q, s):
        return main.at[q, pl.ds(pl.multiple_of(s * rows, rows), rows)]

    def near(q, way):
        return pltpu.make_async_remote_copy(
            src_ref=shard(q, fld),
            dst_ref=shard(q, fld),
            send_sem=ring_send.at[way, q],
            recv_sem=ring_recv.at[way, q],
            device_id=(lat, lax.rem(fld + (1 if way == 0 else NFLD - 1), NFLD)),
            device_id_type=MESH,
        )

    def far(q, way):
        s = lax.rem(fld + (NFLD - 1 if way == 0 else 1), NFLD)
        return pltpu.make_async_remote_copy(
            src_ref=shard(q, s),
            dst_ref=shard(q, s),
            send_sem=relay_send.at[q],
            recv_sem=relay_recv.at[q],
            device_id=(lat, lax.rem(fld + (1 if way == 0 else NFLD - 1), NFLD)),
            device_id_type=MESH,
        )

    def extra_copy(k):
        part = extra.at[pl.ds(pl.multiple_of(fld * rows, rows), rows)]
        return pltpu.make_async_remote_copy(
            src_ref=part,
            dst_ref=part,
            send_sem=extra_send.at[k - 1],
            recv_sem=extra_recv.at[k - 1],
            device_id=(lat, lax.rem(fld + k, NFLD)),
            device_id_type=MESH,
        )

    def start_near(q, carry):
        near(q, 0).start()
        near(q, 1).start()
        return carry

    lax.fori_loop(0, PAIR, start_near, 0)
    for k in range(1, NFLD):
        extra_copy(k).start()
    start_exchange(y, x, send_sem, recv_sem, own_sem)

    def relay(h, carry):
        near(2 * h, 0).wait_recv()
        far(2 * h, 0).start()
        near(2 * h + 1, 1).wait_recv()
        far(2 * h + 1, 1).start()
        return carry

    lax.fori_loop(0, PAIR // 2, relay, 0)
    end_exchange(y, x, send_sem, recv_sem, own_sem)
    for k in range(1, NFLD):
        extra_copy(k).wait()

    def finish(h, carry):
        near(2 * h + 1, 0).wait_recv()
        near(2 * h, 1).wait_recv()
        for way in range(2):
            near(2 * h, way).wait_send()
            near(2 * h + 1, way).wait_send()
        far(2 * h, 0).wait()
        far(2 * h + 1, 1).wait()
        return carry

    lax.fori_loop(0, PAIR // 2, finish, 0)


def move(y, main, extra):
    hbm = pl.BlockSpec(memory_space=pltpu.HBM)
    dma = pltpu.SemaphoreType.DMA
    return pl.pallas_call(
        move_kernel,
        in_specs=[hbm] * 3,
        out_specs=[hbm] * 3,
        out_shape=[jax.ShapeDtypeStruct(a.shape, a.dtype) for a in (y, main, extra)],
        input_output_aliases={1: 1, 2: 2},
        scratch_shapes=[
            dma((NLAT - 1,)), dma((NLAT - 1,)), dma,
            dma((2, PAIR)), dma((2, PAIR)), dma((PAIR,)), dma((PAIR,)),
            dma((NFLD - 1,)), dma((NFLD - 1,)),
        ],
        compiler_params=pltpu.CompilerParams(collective_id=0, has_side_effects=True),
    )(y, main, extra)


def gather_lanes(pieces, width, offset, tile, lane):
    first, last = 128 * tile // width, min((128 * tile + 127) // width, len(pieces) - 1)
    total = None
    for l in range(first, last + 1):
        turned = pltpu.roll(pieces[l](), (width * l - offset) % 128, 1)
        start = width * l - 128 * tile
        total = turned if total is None else jnp.where(lane >= start, turned, total)
    return total


def strided(ref, lead, tiles, first, count, step):
    parts = [ref[lead, k, pl.ds(first, count, stride=step), :] for k in range(tiles)]
    return jnp.concatenate(parts, axis=1)


def legendre_kernel(
    x_ref, a_ref, e_ref, m_ref, s1_ref, s2_ref, s3_ref, spec_ref, out_ref,
    folded, wide, joined, levels, turned,
):
    q = pl.program_id(0)
    half = NLAT // 2

    @pl.when(q == 0)
    def _():
        levels[...] = jnp.zeros_like(levels)
        turned[...] = jnp.zeros_like(turned)
        lane = lax.broadcasted_iota(jnp.int32, (48, 128), 1)

        def tile_of_fields(ft, carry):
            lanes = pl.ds(pl.multiple_of(ft * 128, 128), 128)
            for l in range(half):
                n = x_ref[l, :, :, lanes].astype(F32).reshape(48, 128)
                s = x_ref[NLAT - 1 - l, :, :, lanes].astype(F32).reshape(48, 128)
                folded[0, l] = n + s
                folded[1, l] = n - s
            for sign in range(2):
                pieces = [lambda l=l: folded[sign, l] for l in range(half)]
                for tile in range(5):
                    for fi in range(3):
                        value = gather_lanes(pieces, ROWS, ROWS * fi, tile, lane)
                        first = pl.multiple_of((3 * ft + fi) * 48, 8)
                        wide[sign, tile, pl.ds(first, 48), :] = value
            return carry

        lax.fori_loop(0, FLD // 3, tile_of_fields, 0)

    def operand(sign):
        parts = []
        for par in range(2):
            for c in range(2):
                parts.append(strided(wide, sign, 5, 24 * par + 2 * q + c, FLD, 48))
        return jnp.concatenate(parts, axis=0).astype(BF16)

    sym, anti = operand(0), operand(1)
    a = a_ref[0]
    lane96 = lax.broadcasted_iota(jnp.int32, (96, 128), 1)
    z_sym = jnp.dot(sym, a[:, 0:256], preferred_element_type=F32)
    z_anti = jnp.dot(anti, a[:, 256:512], preferred_element_type=F32)
    z_tail = jnp.where(
        lane96 < 64,
        jnp.dot(sym, a[:, 512:640], preferred_element_type=F32),
        jnp.dot(anti, a[:, 512:640], preferred_element_type=F32),
    )
    z_extra = jnp.dot(sym, e_ref[...], preferred_element_type=F32)
    z_extra = jnp.sum(jnp.where(lane96 == q, z_extra, 0.0), axis=1, keepdims=True)
    mask = m_ref[0]

    def choose(z, row, first):
        even_first = mask[row : row + 1, first : first + z.shape[1]] > 0.5
        return jnp.where(even_first, z[0:48], z[48:96])

    z_sym = choose(z_sym, 0, 0).astype(BF16)
    z_anti = choose(z_anti, 0, 256).astype(BF16)
    z_tail = choose(z_tail, 0, 512).astype(BF16).astype(F32)
    z_extra = choose(jnp.broadcast_to(z_extra, (96, 128)), 1, 0)
    lane = lax.broadcasted_iota(jnp.int32, (48, 128), 1)
    sym32, anti32 = z_sym.astype(F32), z_anti.astype(F32)
    low, high = pltpu.roll(anti32[:, 0:128], 65, 1), pltpu.roll(anti32[:, 128:256], 65, 1)
    end = pltpu.roll(z_tail, 1, 1)
    own = pl.ds(pl.multiple_of(q * 48, 48), 48)
    joined[0, 0, own] = sym32[:, 0:128]
    joined[0, 1, own] = sym32[:, 128:256]
    joined[0, 2, own] = jnp.where(lane < 64, z_tail, jnp.where(lane == 64, z_extra, low))
    joined[0, 3, own] = jnp.where(lane < 65, low, high)
    joined[0, 4, own] = jnp.where(lane < 65, high, end)
    joined[0, 5, own] = end

    zero = jnp.zeros((), BF16)
    for level, (s_ref, place) in enumerate(((s1_ref, 0), (s2_ref, 3), (s3_ref, 5))):
        size = LEVELS[level]
        h = size // 2
        keep = mask[2 + level : 3 + level]
        kept_sym = jnp.where(keep[:, 0:h] > 0.5, z_sym[:, 0:h], zero)
        kept_anti = jnp.where(keep[:, 256 : 256 + h] > 0.5, z_anti[:, 0:h], zero)
        even = jnp.dot(kept_sym, s_ref[0, 0], preferred_element_type=F32)
        odd = jnp.dot(kept_anti, s_ref[0, 1], preferred_element_type=F32)
        for sign, value in enumerate((even + odd, even - odd)):
            for k in range(0, size, 128):
                width = min(128, size - k)
                levels[sign, place + k // 128, own, 0:width] = value[:, k : k + width]

    @pl.when(q == PAIR - 1)
    def _():
        def field(f, carry):
            rows = strided(joined, 0, 6, f, 2 * PAIR, FLD)
            spec_ref[f] = rows[:, 0:641].reshape(PAIR, 2, 641).astype(BF16)
            return carry

        lax.fori_loop(0, FLD, field, 0)
        row = lax.broadcasted_iota(jnp.int32, (640, 1), 0).astype(F32)
        lane_of = lax.broadcasted_iota(jnp.int32, (640, 768), 1).astype(F32)
        block = jnp.floor((row + 0.5) * (1.0 / 40))
        t = row - 40.0 * block
        for sign in range(2):
            for f in range(FLD):
                first = 128 * (f // 6) + 20 * (f % 6)
                turned[first : first + 20] = strided(levels, sign, 6, f, 2 * PAIR, FLD)
            at = [t, t - 24.0, t - 34.0]
            if sign == 1:
                at = [19.0 - t, 33.0 - t, 38.0 - t]
            target = jnp.where(
                t < 20.0,
                20.0 * block + at[0],
                jnp.where(
                    (t >= 24.0) & (t < 34.0),
                    384.0 + 10.0 * block + at[1],
                    jnp.where((t >= 34.0) & (t < 39.0), 640.0 + 5.0 * block + at[2], -1.0),
                ),
            )
            picker = jnp.where(lane_of == target, 1.0, 0.0).astype(BF16)
            picked = lax.dot_general(
                picker, turned[...].astype(BF16), NT, preferred_element_type=F32
            )
            picked = picked.reshape(half, 40, 512).astype(BF16)
            if sign == 0:
                out_ref[0:half] = picked
            else:
                for m in range(half):
                    out_ref[NLAT - 1 - m] = picked[m]


def legendre_step(x, main, extra, masks, synths):
    depth = main.shape[1]
    synth_specs = [
        pl.BlockSpec((1, 2, m // 2, m), lambda q: (q, 0, 0, 0)) for m in LEVELS
    ]
    synths = [s.reshape(PAIR, 2, m // 2, m) for s, m in zip(synths, LEVELS)]
    return pl.pallas_call(
        legendre_kernel,
        grid=(PAIR,),
        in_specs=[
            pl.BlockSpec((NLAT, 2, 24, 1024), lambda q: (0, 0, 0, 0)),
            pl.BlockSpec((1, depth, 640), lambda q: (q, 0, 0)),
            pl.BlockSpec((depth, 128), lambda q: (0, 0)),
            pl.BlockSpec((1, 8, 640), lambda q: (q, 0, 0)),
            *synth_specs,
        ],
        out_specs=[
            pl.BlockSpec((FLD, PAIR, 2, 641), lambda q: (0, 0, 0, 0)),
            pl.BlockSpec((NLAT, 40, 512), lambda q: (0, 0, 0)),
        ],
        out_shape=[
            jax.ShapeDtypeStruct((FLD, PAIR, 2, 641), BF16),
            jax.ShapeDtypeStruct((NLAT, 40, 512), BF16),
        ],
        scratch_shapes=[
            pltpu.VMEM((2, NLAT // 2, 48, 128), F32),
            pltpu.VMEM((2, 5, 48 * FLD, 128), F32),
            pltpu.VMEM((1, 6, 48 * PAIR, 128), F32),
            pltpu.VMEM((2, 6, 48 * PAIR, 128), F32),
            pltpu.VMEM((512, 768), F32),
        ],
    )(x, main, extra, masks, *synths)


def inverse_kernel(cols_ref, b_ref, o1_ref, o2_ref, o3_ref, t1, t2, t3, wide):
    def block(b, carry):
        first = pl.multiple_of(b * 64, 64)
        for table, size, tiles in ((t1, 1280, 10), (t2, 640, 5), (t3, 320, 3)):

            def store(a, value, table=table):
                table[pl.ds(first, 64), 128 * a : 128 * a + 128] = value.astype(BF16)

            fill_table(cols_ref, first, 64, size, 1.0 / math.sqrt(size), tiles, store)
        return carry

    lax.fori_loop(0, 10, block, 0)
    lane = lax.broadcasted_iota(jnp.int32, (40, 128), 1)

    def group(g, carry):
        lanes = pl.ds(pl.multiple_of(g * 128, 128), 128)
        pieces = [lambda l=l: b_ref[l, :, lanes].astype(F32) for l in range(NLAT)]
        for tile in range(5):
            for fi in range(6):
                value = gather_lanes(pieces, 20, 20 * fi, tile, lane)
                first = pl.multiple_of((6 * g + fi) * 40, 8)
                wide[0, tile, pl.ds(first, 40), :] = value
        return carry

    lax.fori_loop(0, 4, group, 0)
    for out_ref, table, start, count in (
        (o1_ref, t1, 0, 20), (o2_ref, t2, 24, 10), (o3_ref, t3, 34, 5)
    ):
        parts = [strided(wide, 0, 5, start + t, FLD, 40) for t in range(count)]
        lhs = jnp.concatenate(parts, axis=0).astype(BF16)
        size = out_ref.shape[2]
        y = jnp.dot(lhs, table[...], preferred_element_type=F32)
        out_ref[...] = y[:, 0:size].reshape(count, FLD, size)


def inverse_step(cols, blocks):
    shapes = [(n, FLD, 4 * m) for n, m in zip(SENT, LEVELS)]
    return pl.pallas_call(
        inverse_kernel,
        in_specs=[pl.BlockSpec(memory_space=pltpu.VMEM)] * 2,
        out_specs=[pl.BlockSpec(memory_space=pltpu.VMEM)] * 3,
        out_shape=[jax.ShapeDtypeStruct(s, F32) for s in shapes],
        scratch_shapes=[
            pltpu.VMEM((640, 1280), BF16),
            pltpu.VMEM((640, 640), BF16),
            pltpu.VMEM((640, 384), BF16),
            pltpu.VMEM((1, 5, 40 * FLD, 128), F32),
        ],
    )(cols, blocks)


def columns(wave, amp, comp):
    parts = [jnp.broadcast_to(v, wave.shape).astype(F32) for v in (wave, amp, comp)]
    return jnp.pad(jnp.stack(parts, axis=-1), ((0, 0), (0, 5)))


def forward_columns(assign):
    even = jnp.where(assign % 2 == 0, assign, 2 * assign.shape[0] - 1 - assign)
    wave = jnp.stack([even, 2 * assign.shape[0] - 1 - even])
    wave = jnp.repeat(wave.reshape(2, NLAT, PAIR), 2, axis=2)
    wave = jnp.pad(wave, ((0, 0), (0, 0), (0, 4))).reshape(-1)
    place = jnp.arange(wave.shape[0]) % 24
    return columns(wave, place < 20, place % 2)


def inverse_columns(assign):
    wave = jnp.repeat(assign, 2)
    return columns(wave, jnp.where(wave == 0, 1.0, 2.0), jnp.arange(wave.shape[0]) % 2)


def mask_rows(own, limits):
    p = own[:, None]
    total = 640
    k = jnp.arange(256)[None, :]
    tail = jnp.arange(64)[None, :] + 256
    first_sym, first_anti = (total + 1 - p) // 2, (total - p) // 2
    zeroth = jnp.concatenate(
        [k < first_sym, k < first_anti, tail < first_sym, tail < first_anti], axis=1
    )
    is_even = p % 2 == 0
    row0 = zeroth == is_even
    row1 = jnp.broadcast_to((320 < first_sym) == is_even, row0.shape)
    rows = [row0, row1]
    for level in range(3):
        keep = [p + 2 * k <= limits[level], p + 1 + 2 * k <= limits[level]]
        rows.append(jnp.concatenate(keep + [jnp.zeros((PAIR, 128), bool)], axis=1))
    stacked = jnp.stack(rows, axis=1).astype(F32)
    return jnp.pad(stacked, ((0, 0), (0, 3), (0, 0)))


def row_turner(lat):
    u = jnp.arange(256)[:, None]
    v = jnp.arange(256)[None, :]
    inner = v % 128
    turned = 128 * (v // 128) + 40 * (inner // 40) + 39 - inner % 40
    source = jnp.where(lat >= NLAT // 2, turned, v)
    return ((u == source) & (inner < 120)).astype(BF16)


def on_device(grid_fields, assign, limits, legendre, synth_one, synth_two, synth_three):
    lat = lax.axis_index("lat")
    fld = lax.axis_index("fld")
    own = lax.dynamic_slice_in_dim(assign, lat * PAIR, PAIR)
    main, extra = pack(jnp.transpose(legendre, (0, 2, 1)), fld.reshape(1))
    y = dft(forward_columns(assign), row_turner(lat), grid_fields)
    x, main, extra = move(y, main, extra)
    spectrum, blocks = legendre_step(
        x, main, extra, mask_rows(own, limits), (synth_one, synth_two, synth_three)
    )
    grids = inverse_step(inverse_columns(assign), exchange(blocks))
    return (
        jnp.transpose(spectrum, (0, 2, 1, 3)),
        *[jnp.transpose(g, (1, 0, 2)) for g in grids],
    )


def solution(mesh):
    return jax.shard_map(
        on_device,
        mesh=mesh,
        in_specs=(
            P("fld", "lat", None),
            P(),
            P(),
            P("lat", None, "fld"),
            P("lat", None, None),
            P("lat", None, None),
            P("lat", None, None),
        ),
        out_specs=(
            P("fld", None, "lat", None),
            P("fld", "lat", None),
            P("fld", "lat", None),
            P("fld", "lat", None),
        ),
        check_vma=False,
    )
```

```python
import math

import jax
import jax.numpy as jnp
from jax import lax
from jax.experimental import pallas as pl
from jax.experimental.pallas import tpu as pltpu
from jax.sharding import PartitionSpec as P

MESH = pl.DeviceIdType.MESH
F32 = jnp.float32
BF16 = jnp.bfloat16
NLAT = 32
NFLD = 4
FLD = 24
ROWS = 40
LON = 2560
PAIR = 10
SENT = (20, 10, 5)
LEVELS = (320, 160, 80)
NT = (((1,), (1,)), ((), ()))


def sincos(turns):
    quarter = jnp.floor(turns * 4.0 + 0.5)
    y = (turns * 4.0 - quarter) * (math.pi / 2)
    y2 = y * y
    s = y * (1.0 + y2 * (-1.0 / 6 + y2 * (1.0 / 120 - y2 * (1.0 / 5040))))
    c = 1.0 + y2 * (-0.5 + y2 * (1.0 / 24 + y2 * (-1.0 / 720 + y2 * (1.0 / 40320))))
    k = quarter - 4.0 * jnp.floor(quarter * 0.25)
    odd = (k == 1.0) | (k == 3.0)
    sin_v = jnp.where(odd, c, s)
    cos_v = jnp.where(odd, s, c)
    sin_v = jnp.where(k >= 2.0, -sin_v, sin_v)
    cos_v = jnp.where((k == 1.0) | (k == 2.0), -cos_v, cos_v)
    return cos_v, sin_v


def turns_of(product, period):
    return (product - period * jnp.floor(product * (1.0 / period))) * (1.0 / period)


def fill_table(cols_ref, first, count, period, scale, tiles, store):
    wave = jnp.broadcast_to(cols_ref[pl.ds(first, count), 0:1], (count, 128))
    amp = jnp.broadcast_to(cols_ref[pl.ds(first, count), 1:2], (count, 128)) * scale
    comp = jnp.broadcast_to(cols_ref[pl.ds(first, count), 2:3], (count, 128))
    lane = lax.broadcasted_iota(jnp.int32, (count, 128), 1).astype(F32)
    cos_v, sin_v = sincos(turns_of(wave * lane + comp * (period // 4), float(period)))
    cos_d, sin_d = sincos(turns_of(wave * 128.0, float(period)))
    cos_v, sin_v = cos_v * amp, sin_v * amp
    for a in range(tiles):
        store(a, cos_v)
        if a + 1 < tiles:
            cos_v, sin_v = cos_v * cos_d - sin_v * sin_d, sin_v * cos_d + cos_v * sin_d


def lat_peer(k):
    return lax.rem(lax.axis_index("lat") + k, NLAT)


def greet():
    barrier = pltpu.get_barrier_semaphore()
    fld = lax.axis_index("fld")
    lat = lax.axis_index("lat")

    def one(k, carry):
        pl.semaphore_signal(barrier, inc=1, device_id=(lat_peer(k), fld), device_id_type=MESH)
        return carry

    lax.fori_loop(1, NLAT, one, 0)
    for k in range(1, NFLD):
        pl.semaphore_signal(
            barrier, inc=1, device_id=(lat, lax.rem(fld + k, NFLD)), device_id_type=MESH
        )
    pl.semaphore_wait(barrier, NLAT + NFLD - 2)


def to_lat(src, dst, send_sem, recv_sem, k):
    return pltpu.make_async_remote_copy(
        src_ref=src,
        dst_ref=dst,
        send_sem=send_sem,
        recv_sem=recv_sem,
        device_id=(lat_peer(k), lax.axis_index("fld")),
        device_id_type=MESH,
    )


def to_fld(part, send_sem, recv_sem, k):
    fld = lax.rem(lax.axis_index("fld") + k, NFLD)
    return pltpu.make_async_remote_copy(
        src_ref=part,
        dst_ref=part,
        send_sem=send_sem,
        recv_sem=recv_sem,
        device_id=(lax.axis_index("lat"), fld),
        device_id_type=MESH,
    )


def each(first, count, act):
    def one(k, carry):
        act(k)
        return carry

    lax.fori_loop(first, count, one, 0)


def pack_pair(q, raw, main, extra, own):
    a = raw[q].astype(F32)
    t = [a[:, 128 * k : 128 * k + 128] for k in range(5)]
    last = a[:, 640:641]
    lane = lax.broadcasted_iota(jnp.int32, (a.shape[0], 128), 1)
    r = [None, None] + [pltpu.roll(t[k], 63, 1) for k in (2, 3, 4)]
    main[q, own, 0:128] = t[0].astype(BF16)
    main[q, own, 128:256] = t[1].astype(BF16)
    main[q, own, 256:384] = jnp.where(lane < 63, r[2], r[3]).astype(BF16)
    main[q, own, 384:512] = jnp.where(lane < 63, r[3], r[4]).astype(BF16)
    tail = jnp.where(lane < 127, pltpu.roll(t[4], 127, 1), last)
    main[q, own, 512:640] = jnp.where(lane < 64, t[2], tail).astype(BF16)
    column = jnp.sum(jnp.where(lane == 64, t[2], 0.0), axis=1, keepdims=True)
    extra[own] = jnp.where(lane == q, column, extra[own].astype(F32)).astype(BF16)


def dft_group(g, table, folded, perm_ref, fields, y_ref, lanes):
    x = fields[pl.ds(g * 6, 6)].astype(F32)
    low = x[:, :, : LON // 2].reshape(240, LON // 2)
    high = x[:, :, LON // 2 :].reshape(240, LON // 2)
    parts = []
    for par in range(2):
        x = low + high if par == 0 else low - high
        folded[0:120] = x[0:120].astype(BF16)
        folded[128:248] = x[120:240].astype(BF16)
        y = lax.dot_general(
            table[768 * par : 768 * par + 768], folded[...], NT, preferred_element_type=F32
        )
        y = jnp.dot(y.astype(BF16), perm_ref[...], preferred_element_type=F32)
        parts.append(y.reshape(NLAT, 24, 256))
    y_ref[:, :, lanes] = jnp.concatenate(parts, axis=1).astype(BF16)


def gather_lanes(pieces, width, offset, tile, lane):
    first, last = 128 * tile // width, min((128 * tile + 127) // width, len(pieces) - 1)
    total = None
    for l in range(first, last + 1):
        turned = pltpu.roll(pieces[l](), (width * l - offset) % 128, 1)
        start = width * l - 128 * tile
        total = turned if total is None else jnp.where(lane >= start, turned, total)
    return total


def strided(ref, lead, tiles, first, count, step):
    parts = [ref[lead, k, pl.ds(first, count, stride=step), :] for k in range(tiles)]
    return jnp.concatenate(parts, axis=1)


def fold_fields(ft, x_ref, folded, wide):
    half = NLAT // 2
    lane = lax.broadcasted_iota(jnp.int32, (48, 128), 1)
    lanes = pl.ds(pl.multiple_of(ft * 128, 128), 128)
    for l in range(half):
        n = x_ref[l, :, lanes].astype(F32)
        s = x_ref[NLAT - 1 - l, :, lanes].astype(F32)
        folded[0, l] = n + s
        folded[1, l] = n - s
    for sign in range(2):
        pieces = [lambda l=l: folded[sign, l] for l in range(half)]
        for tile in range(5):
            for fi in range(3):
                value = gather_lanes(pieces, ROWS, ROWS * fi, tile, lane)
                first = pl.multiple_of((3 * ft + fi) * 48, 8)
                wide[sign, tile, pl.ds(first, 48), :] = value


def legendre_pair(q, wide, main, extra, masks, synths, joined, levels):
    def operand(sign):
        parts = []
        for par in range(2):
            for c in range(2):
                parts.append(strided(wide, sign, 5, 24 * par + 2 * q + c, FLD, 48))
        return jnp.concatenate(parts, axis=0).astype(BF16)

    sym, anti = operand(0), operand(1)
    lane96 = lax.broadcasted_iota(jnp.int32, (96, 128), 1)
    z_sym = jnp.dot(sym, main[q, :, 0:256], preferred_element_type=F32)
    z_anti = jnp.dot(anti, main[q, :, 256:512], preferred_element_type=F32)
    tail = main[q, :, 512:640]
    z_tail = jnp.where(
        lane96 < 64,
        jnp.dot(sym, tail, preferred_element_type=F32),
        jnp.dot(anti, tail, preferred_element_type=F32),
    )
    z_extra = jnp.dot(sym, extra[...], preferred_element_type=F32)
    z_extra = jnp.sum(jnp.where(lane96 == q, z_extra, 0.0), axis=1, keepdims=True)
    mask = masks[q]

    def choose(z, row, first):
        even_first = mask[row : row + 1, first : first + z.shape[1]] > 0.5
        return jnp.where(even_first, z[0:48], z[48:96])

    z_sym = choose(z_sym, 0, 0).astype(BF16)
    z_anti = choose(z_anti, 0, 256).astype(BF16)
    z_tail = choose(z_tail, 0, 512).astype(BF16).astype(F32)
    z_extra = choose(jnp.broadcast_to(z_extra, (96, 128)), 1, 0)
    lane = lax.broadcasted_iota(jnp.int32, (48, 128), 1)
    sym32, anti32 = z_sym.astype(F32), z_anti.astype(F32)
    low, high = pltpu.roll(anti32[:, 0:128], 65, 1), pltpu.roll(anti32[:, 128:256], 65, 1)
    end = pltpu.roll(z_tail, 1, 1)
    own = pl.ds(pl.multiple_of(q * 48, 48), 48)
    joined[0, 0, own] = sym32[:, 0:128]
    joined[0, 1, own] = sym32[:, 128:256]
    joined[0, 2, own] = jnp.where(lane < 64, z_tail, jnp.where(lane == 64, z_extra, low))
    joined[0, 3, own] = jnp.where(lane < 65, low, high)
    joined[0, 4, own] = jnp.where(lane < 65, high, end)
    joined[0, 5, own] = end

    zero = jnp.zeros((), BF16)
    for level, place in enumerate((0, 3, 5)):
        size = LEVELS[level]
        h = size // 2
        keep = mask[2 + level : 3 + level]
        kept_sym = jnp.where(keep[:, 0:h] > 0.5, z_sym[:, 0:h], zero)
        kept_anti = jnp.where(keep[:, 256 : 256 + h] > 0.5, z_anti[:, 0:h], zero)
        even = jnp.dot(kept_sym, synths[level][q, 0], preferred_element_type=F32)
        odd = jnp.dot(kept_anti, synths[level][q, 1], preferred_element_type=F32)
        for sign, value in enumerate((even + odd, even - odd)):
            for k in range(0, size, 128):
                width = min(128, size - k)
                levels[sign, place + k // 128, own, 0:width] = value[:, k : k + width]


def turn_levels(levels, turned, blocks):
    half = NLAT // 2
    row = lax.broadcasted_iota(jnp.int32, (640, 1), 0).astype(F32)
    lane_of = lax.broadcasted_iota(jnp.int32, (640, 768), 1).astype(F32)
    block = jnp.floor((row + 0.5) * (1.0 / 40))
    t = row - 40.0 * block
    for sign in range(2):
        for f in range(FLD):
            first = 128 * (f // 6) + 20 * (f % 6)
            turned[first : first + 20] = strided(levels, sign, 6, f, 2 * PAIR, FLD)
        at = [t, t - 24.0, t - 34.0]
        if sign == 1:
            at = [19.0 - t, 33.0 - t, 38.0 - t]
        target = jnp.where(
            t < 20.0,
            20.0 * block + at[0],
            jnp.where(
                (t >= 24.0) & (t < 34.0),
                384.0 + 10.0 * block + at[1],
                jnp.where((t >= 34.0) & (t < 39.0), 640.0 + 5.0 * block + at[2], -1.0),
            ),
        )
        picker = jnp.where(lane_of == target, 1.0, 0.0).astype(BF16)
        picked = lax.dot_general(picker, turned[...].astype(BF16), NT, preferred_element_type=F32)
        picked = picked.reshape(half, 40, 512).astype(BF16)
        if sign == 0:
            blocks[0:half] = picked
        else:
            for m in range(half):
                blocks[NLAT - 1 - m] = picked[m]


def main_kernel(
    cols, icols, perm, masks, fields_in, legendre_in, s1_in, s2_in, s3_in,
    spec_out, blocks_out, t1_out, t2_out, t3_out,
    raw, main, extra, table, fields, folded_rows, y, x, folded, wide, joined, levels, turned,
    spec, blocks, s1, s2, s3, t1, t2, t3,
    raw_sem, field_sem, load_sem, store_sem, y_send, y_recv, near_send, near_recv,
    far_send, far_recv, extra_send, extra_recv, block_send, block_recv,
):
    lat = lax.axis_index("lat")
    fld = lax.axis_index("fld")
    rows = legendre_in.shape[1]
    own = pl.ds(pl.multiple_of(fld * rows, rows), rows)
    synths = (s1, s2, s3)

    def raw_copy(q):
        return pltpu.make_async_copy(legendre_in.at[q], raw.at[q], raw_sem.at[q])

    def field_copy(g):
        part = pl.ds(g * 6, 6)
        return pltpu.make_async_copy(fields_in.at[part], fields.at[part], field_sem.at[g])

    loads = [
        pltpu.make_async_copy(a, b, load_sem.at[k])
        for k, (a, b) in enumerate(((s1_in, s1), (s2_in, s2), (s3_in, s3)))
    ]
    tables = [
        pltpu.make_async_copy(a, b, store_sem.at[k])
        for k, (a, b) in enumerate(((t1, t1_out), (t2, t2_out), (t3, t3_out)))
    ]
    each(0, PAIR, lambda q: raw_copy(q).start())
    each(0, 4, lambda g: field_copy(g).start())
    for copy in loads:
        copy.start()
    extra[...] = jnp.zeros_like(extra)
    levels[...] = jnp.zeros_like(levels)
    turned[...] = jnp.zeros_like(turned)
    folded_rows[...] = jnp.zeros_like(folded_rows)
    greet()

    def shard(q, k):
        s = lax.rem(fld + k, NFLD)
        return main.at[q, pl.ds(pl.multiple_of(s * rows, rows), rows)]

    step = (1, NFLD - 1)

    def near(q, way):
        return to_fld(shard(q, 0), near_send.at[way, q], near_recv.at[way, q], step[way])

    def far(q, way):
        return to_fld(shard(q, step[1 - way]), far_send.at[q], far_recv.at[q], step[way])

    def extra_copy(k):
        return to_fld(extra.at[own], extra_send.at[k - 1], extra_recv.at[k - 1], k)

    def start_near(q):
        near(q, 0).start()
        near(q, 1).start()

    def pack_one(q):
        raw_copy(q).wait()
        pack_pair(q, raw, main, extra, own)

    pack_one(0)
    pack_one(1)
    start_near(0)

    def fill(b):
        first = pl.multiple_of(b * 64, 64)

        def store(a, value):
            table[pl.ds(first, 64), 128 * a : 128 * a + 128] = value.astype(BF16)

        fill_table(cols, first, 64, LON, 1.0 / math.sqrt(LON), 10, store)

    each(0, 24, fill)
    start_near(1)

    def lanes_of(g):
        return pl.ds(pl.multiple_of(g * 256, 256), 256)

    def y_copy(g, k):
        return to_lat(
            y.at[lat_peer(k), :, lanes_of(g)],
            x.at[lat, :, lanes_of(g)],
            y_send.at[g, k - 1],
            y_recv.at[g, k - 1],
            k,
        )

    def group(g):
        field_copy(g).wait()
        dft_group(g, table, folded_rows, perm, fields, y, lanes_of(g))
        x[lat, :, lanes_of(g)] = y[lat, :, lanes_of(g)]
        pack_one(2 * g + 2)
        pack_one(2 * g + 3)
        each(1, NLAT, lambda k: y_copy(g, k).start())
        start_near(2 * g + 2)
        start_near(2 * g + 3)

    each(0, 4, group)
    for k in range(1, NFLD):
        extra_copy(k).start()

    def fill_inverse(b):
        first = pl.multiple_of(b * 64, 64)
        for out, size, tiles in ((t1, 1280, 10), (t2, 640, 5), (t3, 320, 3)):

            def store(a, value, out=out):
                out[pl.ds(first, 64), 128 * a : 128 * a + 128] = value.astype(BF16)

            fill_table(icols, first, 64, size, 1.0 / math.sqrt(size), tiles, store)

    each(0, 10, fill_inverse)

    def relay(h):
        near(2 * h, 0).wait_recv()
        far(2 * h, 0).start()
        near(2 * h + 1, 1).wait_recv()
        far(2 * h + 1, 1).start()

    each(0, PAIR // 2, relay)
    for copy in tables:
        copy.start()
    for copy in loads:
        copy.wait()
    for k in range(1, NFLD):
        extra_copy(k).wait()

    def arrived(g):
        each(1, NLAT, lambda k: y_copy(g, k).wait())
        fold_fields(2 * g, x, folded, wide)
        fold_fields(2 * g + 1, x, folded, wide)

    each(0, 4, arrived)

    def pairs(h):
        near(2 * h, 1).wait_recv()
        far(2 * h, 0).wait_recv()
        legendre_pair(2 * h, wide, main, extra, masks, synths, joined, levels)
        near(2 * h + 1, 0).wait_recv()
        far(2 * h + 1, 1).wait_recv()
        legendre_pair(2 * h + 1, wide, main, extra, masks, synths, joined, levels)

    each(0, PAIR // 2, pairs)
    turn_levels(levels, turned, blocks)

    def block_copy(k):
        return to_lat(
            blocks.at[lat_peer(k)],
            blocks_out.at[lat],
            block_send.at[k - 1],
            block_recv.at[k - 1],
            k,
        )

    each(1, NLAT, lambda k: block_copy(k).start())
    own_block = pltpu.make_async_copy(blocks.at[lat], blocks_out.at[lat], store_sem.at[3])
    own_block.start()

    def field(f):
        part = strided(joined, 0, 6, f, 2 * PAIR, FLD)
        spec[f] = part[:, 0:641].reshape(PAIR, 2, 641).astype(BF16)

    each(0, FLD, field)
    spec_copy = pltpu.make_async_copy(spec, spec_out, store_sem.at[4])
    spec_copy.start()

    def sent(h):
        for way in range(2):
            near(2 * h, way).wait_send()
            near(2 * h + 1, way).wait_send()
        far(2 * h, 0).wait_send()
        far(2 * h + 1, 1).wait_send()

    each(0, PAIR // 2, sent)
    for copy in tables:
        copy.wait()
    each(1, NLAT, lambda k: block_copy(k).wait())
    own_block.wait()
    spec_copy.wait()


def main_step(cols, icols, perm, masks, fields, legendre_t, synths):
    hbm = pl.BlockSpec(memory_space=pltpu.HBM)
    vmem = pl.BlockSpec(memory_space=pltpu.VMEM)
    dma = pltpu.SemaphoreType.DMA
    rows = legendre_t.shape[1]
    synths = [s.reshape(PAIR, 2, m // 2, m) for s, m in zip(synths, LEVELS)]
    wides = (1280, 640, 384)
    return pl.pallas_call(
        main_kernel,
        in_specs=[vmem] * 4 + [hbm] * 5,
        out_specs=[hbm] * 5,
        out_shape=[
            jax.ShapeDtypeStruct((FLD, PAIR, 2, 641), BF16),
            jax.ShapeDtypeStruct((NLAT, 40, 512), BF16),
            *[jax.ShapeDtypeStruct((640, w), BF16) for w in wides],
        ],
        scratch_shapes=[
            pltpu.VMEM((PAIR, rows, 641), BF16),
            pltpu.VMEM((PAIR, NFLD * rows, 640), BF16),
            pltpu.VMEM((NFLD * rows, 128), BF16),
            pltpu.VMEM((1536, LON // 2), BF16),
            pltpu.VMEM((FLD, ROWS, LON), BF16),
            pltpu.VMEM((256, LON // 2), BF16),
            pltpu.VMEM((NLAT, 48, 1024), BF16),
            pltpu.VMEM((NLAT, 48, 1024), BF16),
            pltpu.VMEM((2, NLAT // 2, 48, 128), F32),
            pltpu.VMEM((2, 5, 48 * FLD, 128), F32),
            pltpu.VMEM((1, 6, 48 * PAIR, 128), F32),
            pltpu.VMEM((2, 6, 48 * PAIR, 128), F32),
            pltpu.VMEM((512, 768), F32),
            pltpu.VMEM((FLD, PAIR, 2, 641), BF16),
            pltpu.VMEM((NLAT, 40, 512), BF16),
            *[pltpu.VMEM(s.shape, BF16) for s in synths],
            *[pltpu.VMEM((640, w), BF16) for w in wides],
            dma((PAIR,)), dma((4,)), dma((3,)), dma((5,)),
            dma((4, NLAT - 1)), dma((4, NLAT - 1)),
            dma((2, PAIR)), dma((2, PAIR)), dma((PAIR,)), dma((PAIR,)),
            dma((NFLD - 1,)), dma((NFLD - 1,)),
            dma((NLAT - 1,)), dma((NLAT - 1,)),
        ],
        compiler_params=pltpu.CompilerParams(
            collective_id=0, has_side_effects=True, vmem_limit_bytes=64 * 1000 * 1000
        ),
    )(cols, icols, perm, masks, fields, legendre_t, *synths)


def inverse_kernel(b_ref, t1, t2, t3, o1_ref, o2_ref, o3_ref, wide):
    lane = lax.broadcasted_iota(jnp.int32, (40, 128), 1)

    def group(g, carry):
        lanes = pl.ds(pl.multiple_of(g * 128, 128), 128)
        pieces = [lambda l=l: b_ref[l, :, lanes].astype(F32) for l in range(NLAT)]
        for tile in range(5):
            for fi in range(6):
                value = gather_lanes(pieces, 20, 20 * fi, tile, lane)
                first = pl.multiple_of((6 * g + fi) * 40, 8)
                wide[0, tile, pl.ds(first, 40), :] = value
        return carry

    lax.fori_loop(0, 4, group, 0)
    for out_ref, table, start, count in (
        (o1_ref, t1, 0, 20), (o2_ref, t2, 24, 10), (o3_ref, t3, 34, 5)
    ):
        parts = [strided(wide, 0, 5, start + t, FLD, 40) for t in range(count)]
        lhs = jnp.concatenate(parts, axis=0).astype(BF16)
        size = out_ref.shape[2]
        y = jnp.dot(lhs, table[...], preferred_element_type=F32)
        out_ref[...] = y[:, 0:size].reshape(count, FLD, size)


def inverse_step(blocks, tables):
    shapes = [(n, FLD, 4 * m) for n, m in zip(SENT, LEVELS)]
    return pl.pallas_call(
        inverse_kernel,
        in_specs=[pl.BlockSpec(memory_space=pltpu.VMEM)] * 4,
        out_specs=[pl.BlockSpec(memory_space=pltpu.VMEM)] * 3,
        out_shape=[jax.ShapeDtypeStruct(s, F32) for s in shapes],
        scratch_shapes=[
            pltpu.VMEM((1, 5, 40 * FLD, 128), F32),
        ],
    )(blocks, *tables)


def columns(wave, amp, comp):
    parts = [jnp.broadcast_to(v, wave.shape).astype(F32) for v in (wave, amp, comp)]
    return jnp.pad(jnp.stack(parts, axis=-1), ((0, 0), (0, 5)))


def forward_columns(assign):
    even = jnp.where(assign % 2 == 0, assign, 2 * assign.shape[0] - 1 - assign)
    wave = jnp.stack([even, 2 * assign.shape[0] - 1 - even])
    wave = jnp.repeat(wave.reshape(2, NLAT, PAIR), 2, axis=2)
    wave = jnp.pad(wave, ((0, 0), (0, 0), (0, 4))).reshape(-1)
    place = jnp.arange(wave.shape[0]) % 24
    return columns(wave, place < 20, place % 2)


def inverse_columns(assign):
    wave = jnp.repeat(assign, 2)
    return columns(wave, jnp.where(wave == 0, 1.0, 2.0), jnp.arange(wave.shape[0]) % 2)


def mask_rows(own, limits):
    p = own[:, None]
    total = 640
    k = jnp.arange(256)[None, :]
    tail = jnp.arange(64)[None, :] + 256
    first_sym, first_anti = (total + 1 - p) // 2, (total - p) // 2
    zeroth = jnp.concatenate(
        [k < first_sym, k < first_anti, tail < first_sym, tail < first_anti], axis=1
    )
    is_even = p % 2 == 0
    row0 = zeroth == is_even
    row1 = jnp.broadcast_to((320 < first_sym) == is_even, row0.shape)
    rows = [row0, row1]
    for level in range(3):
        keep = [p + 2 * k <= limits[level], p + 1 + 2 * k <= limits[level]]
        rows.append(jnp.concatenate(keep + [jnp.zeros((PAIR, 128), bool)], axis=1))
    stacked = jnp.stack(rows, axis=1).astype(F32)
    return jnp.pad(stacked, ((0, 0), (0, 3), (0, 0)))


def row_turner(lat):
    u = jnp.arange(256)[:, None]
    v = jnp.arange(256)[None, :]
    inner = v % 128
    turned = 128 * (v // 128) + 40 * (inner // 40) + 39 - inner % 40
    source = jnp.where(lat >= NLAT // 2, turned, v)
    return ((u == source) & (inner < 120)).astype(BF16)


def on_device(grid_fields, assign, limits, legendre, synth_one, synth_two, synth_three):
    lat = lax.axis_index("lat")
    own = lax.dynamic_slice_in_dim(assign, lat * PAIR, PAIR)
    spectrum, blocks, *tables = main_step(
        forward_columns(assign),
        inverse_columns(assign),
        row_turner(lat),
        mask_rows(own, limits),
        grid_fields,
        jnp.transpose(legendre, (0, 2, 1)),
        (synth_one, synth_two, synth_three),
    )
    grids = inverse_step(blocks, tables)
    return (
        jnp.transpose(spectrum, (0, 2, 1, 3)),
        *[jnp.transpose(g, (1, 0, 2)) for g in grids],
    )


def solution(mesh):
    return jax.shard_map(
        on_device,
        mesh=mesh,
        in_specs=(
            P("fld", "lat", None),
            P(),
            P(),
            P("lat", None, "fld"),
            P("lat", None, None),
            P("lat", None, None),
            P("lat", None, None),
        ),
        out_specs=(
            P("fld", None, "lat", None),
            P("fld", "lat", None),
            P("fld", "lat", None),
            P("fld", "lat", None),
        ),
        check_vma=False,
    )
```

```python
import math

import jax
import jax.numpy as jnp
from jax import lax
from jax.experimental import pallas as pl
from jax.experimental.pallas import tpu as pltpu
from jax.sharding import PartitionSpec as P

MESH = pl.DeviceIdType.MESH
F32 = jnp.float32
BF16 = jnp.bfloat16
NLAT = 32
NFLD = 4
FLD = 24
ROWS = 40
LON = 2560
PAIR = 10
SENT = (20, 10, 5)
LEVELS = (320, 160, 80)
NT = (((1,), (1,)), ((), ()))
EARLY = 8
DEEP = 2 * EARLY * NLAT


def sincos(turns):
    quarter = jnp.floor(turns * 4.0 + 0.5)
    y = (turns * 4.0 - quarter) * (math.pi / 2)
    y2 = y * y
    s = y * (1.0 + y2 * (-1.0 / 6 + y2 * (1.0 / 120 - y2 * (1.0 / 5040))))
    c = 1.0 + y2 * (-0.5 + y2 * (1.0 / 24 + y2 * (-1.0 / 720 + y2 * (1.0 / 40320))))
    k = quarter - 4.0 * jnp.floor(quarter * 0.25)
    odd = (k == 1.0) | (k == 3.0)
    sin_v = jnp.where(odd, c, s)
    cos_v = jnp.where(odd, s, c)
    sin_v = jnp.where(k >= 2.0, -sin_v, sin_v)
    cos_v = jnp.where((k == 1.0) | (k == 2.0), -cos_v, cos_v)
    return cos_v, sin_v


def turns_of(product, period):
    return (product - period * jnp.floor(product * (1.0 / period))) * (1.0 / period)


def fill_table(cols_ref, first, count, period, scale, tiles, store):
    wave = jnp.broadcast_to(cols_ref[pl.ds(first, count), 0:1], (count, 128))
    amp = jnp.broadcast_to(cols_ref[pl.ds(first, count), 1:2], (count, 128)) * scale
    comp = jnp.broadcast_to(cols_ref[pl.ds(first, count), 2:3], (count, 128))
    lane = lax.broadcasted_iota(jnp.int32, (count, 128), 1).astype(F32)
    cos_v, sin_v = sincos(turns_of(wave * lane + comp * (period // 4), float(period)))
    cos_d, sin_d = sincos(turns_of(wave * 128.0, float(period)))
    cos_v, sin_v = cos_v * amp, sin_v * amp
    for a in range(tiles):
        store(a, cos_v)
        if a + 1 < tiles:
            cos_v, sin_v = cos_v * cos_d - sin_v * sin_d, sin_v * cos_d + cos_v * sin_d


def lat_peer(k):
    return lax.rem(lax.axis_index("lat") + k, NLAT)


def greet():
    barrier = pltpu.get_barrier_semaphore()
    fld = lax.axis_index("fld")
    lat = lax.axis_index("lat")

    def one(k, carry):
        pl.semaphore_signal(barrier, inc=1, device_id=(lat_peer(k), fld), device_id_type=MESH)
        return carry

    lax.fori_loop(1, NLAT, one, 0)
    for k in range(1, NFLD):
        pl.semaphore_signal(
            barrier, inc=1, device_id=(lat, lax.rem(fld + k, NFLD)), device_id_type=MESH
        )
    return lambda: pl.semaphore_wait(barrier, NLAT + NFLD - 2)


def to_lat(src, dst, send_sem, recv_sem, k):
    return pltpu.make_async_remote_copy(
        src_ref=src,
        dst_ref=dst,
        send_sem=send_sem,
        recv_sem=recv_sem,
        device_id=(lat_peer(k), lax.axis_index("fld")),
        device_id_type=MESH,
    )


def to_fld(part, send_sem, recv_sem, k):
    fld = lax.rem(lax.axis_index("fld") + k, NFLD)
    return pltpu.make_async_remote_copy(
        src_ref=part,
        dst_ref=part,
        send_sem=send_sem,
        recv_sem=recv_sem,
        device_id=(lax.axis_index("lat"), fld),
        device_id_type=MESH,
    )


def each(first, count, act):
    def one(k, carry):
        act(k)
        return carry

    lax.fori_loop(first, count, one, 0)


def pack_pair(q, raw, main, extra, own):
    a = raw[q].astype(F32)
    t = [a[:, 128 * k : 128 * k + 128] for k in range(5)]
    last = a[:, 640:641]
    lane = lax.broadcasted_iota(jnp.int32, (a.shape[0], 128), 1)
    r = [None, None] + [pltpu.roll(t[k], 63, 1) for k in (2, 3, 4)]
    main[q, own, 0:128] = t[0].astype(BF16)
    main[q, own, 128:256] = t[1].astype(BF16)
    main[q, own, 256:384] = jnp.where(lane < 63, r[2], r[3]).astype(BF16)
    main[q, own, 384:512] = jnp.where(lane < 63, r[3], r[4]).astype(BF16)
    tail = jnp.where(lane < 127, pltpu.roll(t[4], 127, 1), last)
    main[q, own, 512:640] = jnp.where(lane < 64, t[2], tail).astype(BF16)
    column = jnp.sum(jnp.where(lane == 64, t[2], 0.0), axis=1, keepdims=True)
    extra[own] = jnp.where(lane == q, column, extra[own].astype(F32)).astype(BF16)


def dft_group(g, table, folded, perm_ref, fields, y_ref, lanes):
    x = fields[pl.ds(g * 6, 6)].astype(F32)
    low = x[:, :, : LON // 2].reshape(240, LON // 2)
    high = x[:, :, LON // 2 :].reshape(240, LON // 2)
    parts = []
    for par in range(2):
        x = low + high if par == 0 else low - high
        folded[0:120] = x[0:120].astype(BF16)
        folded[128:248] = x[120:240].astype(BF16)
        y = lax.dot_general(
            table[768 * par : 768 * par + 768], folded[...], NT, preferred_element_type=F32
        )
        y = jnp.dot(y.astype(BF16), perm_ref[...], preferred_element_type=F32)
        parts.append((y[0:512].reshape(NLAT, 16, 256), y[512:768].reshape(NLAT, 8, 256)))
    (first, mid), (last, other) = parts
    y_ref[:, :, lanes] = jnp.concatenate([first, mid + other, last], axis=1).astype(BF16)


def make_columns(assign_ref, cols, part):
    p = assign_ref[...].reshape(1, -1).astype(F32)
    total = 2.0 * assign_ref.shape[0] - 1.0
    even = jnp.where(p - 2.0 * jnp.floor(p * 0.5) > 0.5, total - p, p)
    value = (even, total - even, p)[part]
    high = jnp.floor(value * (1.0 / 16))
    place = lax.broadcasted_iota(jnp.int32, (8, value.shape[1]), 0)
    digits = jnp.where(place == 0, high, jnp.where(place == 1, value - 16.0 * high, 0.0))
    r = lax.broadcasted_iota(jnp.int32, (768, 1), 0).astype(F32)
    if part < 2:
        rest = r >= 512.0
        s = jnp.where(rest, r - 512.0, r)
        l = jnp.where(rest, jnp.floor((s + 0.5) * (1.0 / 8)), jnp.floor((s + 0.5) * (1.0 / 16)))
        i = s - jnp.where(rest, 8.0, 16.0) * l
        if part == 0:
            valid = jnp.logical_not(rest) | (i < 4.0)
            q = jnp.floor(i * 0.5) + jnp.where(rest, 8.0, 0.0)
        else:
            valid = jnp.logical_not(rest) | (i >= 4.0)
            q = jnp.floor(i * 0.5) + jnp.where(rest, 6.0, 0.0)
    else:
        late = r >= 512.0
        s = jnp.where(late, r - 512.0, r)
        valid = r < 640.0
        l = jnp.where(late, jnp.floor((s + 0.5) * 0.25), jnp.floor((s + 0.5) * (1.0 / 16)))
        i = s - jnp.where(late, 4.0, 16.0) * l
        q = jnp.floor(i * 0.5) + jnp.where(late, 8.0, 0.0)
    slot = jnp.where(valid, 10.0 * l + q, -1.0)
    lane = lax.broadcasted_iota(jnp.int32, (768, value.shape[1]), 1).astype(F32)
    picker = jnp.where(lane == slot, 1.0, 0.0).astype(BF16)
    found = lax.dot_general(picker, digits.astype(BF16), NT, preferred_element_type=F32)
    wave = 16.0 * found[:, 0:1] + found[:, 1:2]
    amp = jnp.where(valid, 1.0, 0.0)
    if part == 2:
        amp = amp * jnp.where(wave > 0.5, 2.0, 1.0)
    rows = slice(768 * part, 768 * part + 768)
    cols[rows, 0:1] = wave
    cols[rows, 1:2] = amp
    cols[rows, 2:3] = r - 2.0 * jnp.floor(r * 0.5)


def make_turner(perm):
    u = lax.broadcasted_iota(jnp.int32, (256, 256), 0).astype(F32)
    v = lax.broadcasted_iota(jnp.int32, (256, 256), 1).astype(F32)
    inner = v - 128.0 * jnp.floor(v * (1.0 / 128))
    t = inner - 40.0 * jnp.floor((inner + 0.5) * (1.0 / 40))
    source = jnp.where(lax.axis_index("lat") >= NLAT // 2, v + 39.0 - 2.0 * t, v)
    perm[...] = jnp.where((u == source) & (inner < 120.0), 1.0, 0.0).astype(BF16)


def gather_lanes(pieces, width, offset, tile, lane):
    first, last = 128 * tile // width, min((128 * tile + 127) // width, len(pieces) - 1)
    total = None
    for l in range(first, last + 1):
        turned = pltpu.roll(pieces[l](), (width * l - offset) % 128, 1)
        start = width * l - 128 * tile
        total = turned if total is None else jnp.where(lane >= start, turned, total)
    return total


def strided(ref, lead, tiles, first, count, step):
    parts = [ref[lead + k, pl.ds(first, count, stride=step), :] for k in range(tiles)]
    return jnp.concatenate(parts, axis=1)


def fold_fields(ft, x_ref, folded, wide):
    half = NLAT // 2
    lane = lax.broadcasted_iota(jnp.int32, (40, 128), 1)
    lanes = pl.ds(pl.multiple_of(ft * 128, 128), 128)
    for l in range(half):
        n = x_ref[l, :, lanes].astype(F32)
        s = x_ref[NLAT - 1 - l, :, lanes].astype(F32)
        folded[0, l] = n + s
        folded[1, l] = n - s
    for sign in range(2):
        pieces = [lambda l=l: folded[sign, l] for l in range(half)]
        for tile in range(5):
            for fi in range(3):
                value = gather_lanes(pieces, ROWS, ROWS * fi, tile, lane)
                first = pl.multiple_of((3 * ft + fi) * 40, 8)
                wide[5 * sign + tile, pl.ds(first, 40), :] = value


def legendre_pair(q, p, limits, wide, main, extra, synths, joined, levels):
    def operand(sign):
        parts = []
        for par in range(2):
            for c in range(2):
                row = 2 * q + c
                if par == 1:
                    row += 24 - 20 * lax.div(q, 8)
                parts.append(strided(wide, 5 * sign, 5, row, FLD, 40))
        return jnp.concatenate(parts, axis=0).astype(BF16)

    sym, anti = operand(0), operand(1)
    lane96 = lax.broadcasted_iota(jnp.int32, (96, 128), 1)
    z_sym = jnp.dot(sym, main[q, :, 0:256], preferred_element_type=F32)
    z_anti = jnp.dot(anti, main[q, :, 256:512], preferred_element_type=F32)
    tail = main[q, :, 512:640]
    z_tail = jnp.where(
        lane96 < 64,
        jnp.dot(sym, tail, preferred_element_type=F32),
        jnp.dot(anti, tail, preferred_element_type=F32),
    )
    z_extra = jnp.dot(sym, extra[...], preferred_element_type=F32)
    z_extra = jnp.sum(jnp.where(lane96 == q, z_extra, 0.0), axis=1, keepdims=True)
    first_sym = lax.shift_right_logical(641 - p, 1)
    first_anti = lax.shift_right_logical(640 - p, 1)
    parity = lax.bitwise_and(p, 1)

    def choose(z, rank, first):
        taken = jnp.where(rank < first, 1, 0) ^ parity
        return jnp.where(taken == 1, z[0:48], z[48:96])

    lane = lax.broadcasted_iota(jnp.int32, (48, 128), 1)
    rank = lax.broadcasted_iota(jnp.int32, (48, 256), 1)
    z_sym = choose(z_sym, rank, first_sym).astype(BF16)
    z_anti = choose(z_anti, rank, first_anti).astype(BF16)
    z_tail = jnp.where(
        lane < 64,
        choose(z_tail, lane + 256, first_sym),
        choose(z_tail, lane + 192, first_anti),
    )
    z_tail = z_tail.astype(BF16).astype(F32)
    z_extra = choose(jnp.broadcast_to(z_extra, (96, 128)), lane * 0 + 320, first_sym)
    sym32, anti32 = z_sym.astype(F32), z_anti.astype(F32)
    low, high = pltpu.roll(anti32[:, 0:128], 65, 1), pltpu.roll(anti32[:, 128:256], 65, 1)
    end = pltpu.roll(z_tail, 1, 1)
    own = pl.ds(pl.multiple_of(q * 48, 48), 48)
    joined[0, own] = sym32[:, 0:128]
    joined[1, own] = sym32[:, 128:256]
    joined[2, own] = jnp.where(lane < 64, z_tail, jnp.where(lane == 64, z_extra, low))
    joined[3, own] = jnp.where(lane < 65, low, high)
    joined[4, own] = jnp.where(lane < 65, high, end)
    joined[5, own] = end

    for level, place in enumerate((0, 3, 5)):
        size = LEVELS[level]
        h = size // 2
        degree = p + 2 * rank
        kept_sym = jnp.where(degree <= limits[level], sym32, 0.0).astype(BF16)[:, 0:h]
        kept_anti = jnp.where(degree + 1 <= limits[level], anti32, 0.0).astype(BF16)[:, 0:h]
        even = jnp.dot(kept_sym, synths[level][q, 0], preferred_element_type=F32)
        odd = jnp.dot(kept_anti, synths[level][q, 1], preferred_element_type=F32)
        for sign, value in enumerate((even + odd, even - odd)):
            for k in range(0, size, 128):
                width = min(128, size - k)
                levels[6 * sign + place + k // 128, own, 0:width] = value[:, k : k + width]


def make_pickers(pickers):
    row = lax.broadcasted_iota(jnp.int32, (640, 1), 0).astype(F32)
    lane_of = lax.broadcasted_iota(jnp.int32, (640, 768), 1).astype(F32)
    block = jnp.floor((row + 0.5) * (1.0 / 40))
    t = row - 40.0 * block
    for sign in range(2):
        at = [t, t - 24.0, t - 34.0]
        if sign == 1:
            at = [19.0 - t, 33.0 - t, 38.0 - t]
        target = jnp.where(
            t < 20.0,
            20.0 * block + at[0],
            jnp.where(
                (t >= 24.0) & (t < 34.0),
                384.0 + 10.0 * block + at[1],
                jnp.where((t >= 34.0) & (t < 39.0), 640.0 + 5.0 * block + at[2], -1.0),
            ),
        )
        pickers[sign] = jnp.where(lane_of == target, 1.0, 0.0).astype(BF16)


def turn_levels(part, levels, turned, pickers, blocks):
    half = NLAT // 2
    count = 2 * (EARLY if part == 0 else PAIR - EARLY)
    base = 0 if part == 0 else 2 * EARLY * FLD
    size = blocks.shape[2]
    for sign in range(2):
        for f in range(FLD):
            value = strided(levels, 6 * sign, 6, base + f, count, FLD)
            turned[base + count * f : base + count * f + count] = value
        picked = lax.dot_general(
            pickers[sign],
            turned[base : base + size].astype(BF16),
            NT,
            preferred_element_type=F32,
        )
        picked = picked.reshape(half, 40, size).astype(BF16)
        if sign == 0:
            blocks[0:half] = picked
        else:
            for m in range(half):
                blocks[NLAT - 1 - m] = picked[m]


def swap_units(values, width):
    lane = lax.broadcasted_iota(jnp.int32, values[0].shape, 1)
    values = list(values)
    k = 1
    while k < len(values):
        upper = (lane & (k * width)) != 0
        for a in range(len(values)):
            if a & k == 0:
                low, high = values[a], values[a + k]
                values[a] = jnp.where(upper, pltpu.roll(high, k * width, 1), low)
                values[a + k] = jnp.where(upper, high, pltpu.roll(low, 128 - k * width, 1))
        k *= 2
    return values


def spread_early(arrived, wide):
    def group(g):
        lanes = pl.ds(pl.multiple_of(g * 128, 128), 128)
        for tile in range(4):
            values = [arrived[8 * tile + a, :, lanes].astype(F32) for a in range(8)]
            for a, value in enumerate(swap_units(values, 16)):
                wide[tile, pl.ds(8 * g + a, 40, stride=FLD), :] = value

    each(0, 3, group)


def spread_late(arrived, wide):
    def rows(b):
        own = pl.ds(pl.multiple_of(8 * b, 8), 8)
        values = [arrived[l, own, :].astype(F32) for l in range(NLAT)]
        for f, value in enumerate(swap_units(values, 4)[0:FLD]):
            wide[4, pl.ds(8 * FLD * b + f, 8, stride=FLD), :] = value

    each(0, 5, rows)


LEVEL_ROWS = ((0, 480), (576, 240), (816, 120))


def main_kernel(
    assign_s, limits, assign_v, fields_in, legendre_in, s1_in, s2_in, s3_in,
    spec_out, rows_out, p1_out, p2_out, p3_out, t1_out, t2_out, t3_out,
    raw, main, extra, table, fields, folded_rows, y, x, folded, wide, joined, levels, turned,
    spec, early, late, early_in, late_in, rows_v, pickers, cols, perm, s1, s2, s3, t1, t2, t3,
    p1, p2, p3,
    raw_sem, field_sem, load_sem, store_sem, y_send, y_recv, near_send, near_recv,
    far_send, far_recv, extra_send, extra_recv, block_send, block_recv,
):
    lat = lax.axis_index("lat")
    fld = lax.axis_index("fld")
    rows = legendre_in.shape[1]
    own = pl.ds(pl.multiple_of(fld * rows, rows), rows)
    synths = (s1, s2, s3)

    def raw_copy(q):
        return pltpu.make_async_copy(legendre_in.at[q], raw.at[q], raw_sem.at[q])

    def field_copy(g):
        part = pl.ds(g * 6, 6)
        return pltpu.make_async_copy(fields_in.at[part], fields.at[part], field_sem.at[g])

    loads = [
        pltpu.make_async_copy(a, b, load_sem.at[k])
        for k, (a, b) in enumerate(((s1_in, s1), (s2_in, s2), (s3_in, s3)))
    ]
    tables = [
        pltpu.make_async_copy(a.at[pl.ds(DEEP, 128)], b, store_sem.at[k])
        for k, (a, b) in enumerate(((t1, t1_out), (t2, t2_out), (t3, t3_out)))
    ]
    each(0, PAIR, lambda q: raw_copy(q).start())
    each(0, 4, lambda g: field_copy(g).start())
    for copy in loads:
        copy.start()
    all_greeted = greet()
    extra[own] = jnp.zeros((rows, 128), BF16)
    folded_rows[...] = jnp.zeros_like(folded_rows)

    def shard(q, k):
        s = lax.rem(fld + k, NFLD)
        return main.at[q, pl.ds(pl.multiple_of(s * rows, rows), rows)]

    def near(h, way):
        pair = main.at[pl.ds(2 * h, 2), own]
        return to_fld(pair, near_send, near_recv.at[way, h], 1 + 2 * way)

    def near_last(q, way):
        return to_fld(shard(q, 0), near_send, near_recv.at[way, q - 4], 1 + 2 * way)

    def far(q, way):
        return to_fld(shard(q, 3 - 2 * way), far_send, far_recv.at[q], 1 + 2 * way)

    def extra_copy(k):
        return to_fld(extra.at[own], extra_send.at[k - 1], extra_recv.at[k - 1], k)

    def start_near(h):
        near(h, 0).start()
        near(h, 1).start()

    def start_last():
        near_last(8, 0).start()
        near_last(9, 1).start()
        near_last(9, 0).start()
        near_last(8, 1).start()

    def pack_one(q):
        raw_copy(q).wait()
        pack_pair(q, raw, main, extra, own)

    pack_one(0)
    pack_one(1)
    all_greeted()
    start_near(0)
    make_columns(assign_v, cols, 0)
    make_columns(assign_v, cols, 1)
    make_turner(perm)

    def fill(b):
        first = pl.multiple_of(b * 64, 64)

        def store(a, value):
            table[pl.ds(first, 64), 128 * a : 128 * a + 128] = value.astype(BF16)

        fill_table(cols, first, 64, LON, 1.0 / math.sqrt(LON), 10, store)

    each(0, 24, fill)
    pack_one(2)
    pack_one(3)

    def lanes_of(g):
        return pl.ds(pl.multiple_of(g * 256, 256), 256)

    def y_copy(g, k):
        return to_lat(
            y.at[lat_peer(k), :, lanes_of(g)],
            x.at[lat, :, lanes_of(g)],
            y_send.at[g],
            y_recv.at[g],
            k,
        )

    def y_wait(g):
        part = pl.ds(0, NLAT - 1)
        both = to_lat(
            y.at[part, :, lanes_of(g)], x.at[part, :, lanes_of(g)], y_send.at[g], y_recv.at[g], 1
        )
        both.wait_send()
        both.wait_recv()

    def relay(h):
        near(h, 0).wait_recv()
        far(2 * h, 0).start()
        near(h, 1).wait_recv()
        far(2 * h + 1, 1).start()

    def transform(g):
        field_copy(g).wait()
        dft_group(g, table, folded_rows, perm, fields, y, lanes_of(g))
        x[lat, :, lanes_of(g)] = y[lat, :, lanes_of(g)]

    def send_group(g):
        each(1, NLAT, lambda k: y_copy(g, k).start())

    def group(g):
        transform(g)
        start_near(g + 1)
        pack_one(2 * g + 4)
        pack_one(2 * g + 5)
        send_group(g)

        @pl.when(g > 0)
        def _():
            relay(g - 1)

    each(0, 3, group)
    transform(3)
    send_group(3)
    for k in range(1, NFLD):
        extra_copy(k).start()

    levels[...] = jnp.zeros_like(levels)
    turned[...] = jnp.zeros_like(turned)
    make_pickers(pickers)
    make_columns(assign_v, cols, 2)

    def fill_inverse(b):
        first = pl.multiple_of(b * 64, 64)
        for out, size, tiles in ((t1, 1280, 10), (t2, 640, 5), (t3, 320, 3)):

            def store(a, value, out=out):
                out[pl.ds(first, 64), 128 * a : 128 * a + 128] = value.astype(BF16)

            fill_table(cols, 1536 + first, 64, size, 1.0 / math.sqrt(size), tiles, store)

    each(0, 12, fill_inverse)
    for copy in tables:
        copy.start()

    def take_group(g):
        y_wait(g)
        fold_fields(2 * g, x, folded, wide)
        fold_fields(2 * g + 1, x, folded, wide)

        @pl.when(g == 0)
        def _():
            relay(2)

        @pl.when(g == 2)
        def _():
            relay(3)
            start_last()

    each(0, 4, take_group)
    for copy in loads:
        copy.wait()
    for k in range(1, NFLD):
        extra_copy(k).wait()

    parts = ((early, early_in), (late, late_in))

    def block_copy(part, k):
        return to_lat(
            parts[part][0].at[lat_peer(k)],
            parts[part][1].at[lat],
            block_send.at[part],
            block_recv.at[part],
            k,
        )

    def pair(q):
        way = lax.rem(q, 2)
        far(q, way).wait_recv()
        p = assign_s[PAIR * lat + q]
        legendre_pair(q, p, limits, wide, main, extra, synths, joined, levels)

    def send_part(part):
        turn_levels(part, levels, turned, pickers, parts[part][0])
        parts[part][1][lat] = parts[part][0][lat]
        each(1, NLAT, lambda k: block_copy(part, k).start())

    def take_part(part):
        count = pl.ds(0, NLAT - 1)
        both = to_lat(
            parts[part][0].at[count], parts[part][1].at[count], block_send.at[part],
            block_recv.at[part], 1,
        )
        both.wait_send()
        both.wait_recv()

    each(0, EARLY, pair)
    send_part(0)
    near_last(8, 0).wait_recv()
    far(8, 0).start()
    near_last(9, 1).wait_recv()
    far(9, 1).start()
    near_last(8, 1).wait_recv()
    near_last(9, 0).wait_recv()
    each(EARLY, PAIR, pair)
    send_part(1)

    def field(f):
        part = strided(joined, 0, 6, f, 2 * PAIR, FLD)
        spec[f] = part[:, 0:641].reshape(PAIR, 2, 641).astype(BF16)

    each(0, FLD, field)
    spec_copy = pltpu.make_async_copy(spec, spec_out, store_sem.at[4])
    spec_copy.start()

    first_two = main.at[:, pl.ds(0, 2 * rows)]
    to_fld(first_two, near_send, near_recv.at[0, 0], 1).wait_send()
    to_fld(main.at[:, pl.ds(0, rows)], far_send, far_recv.at[0], 1).wait_send()
    take_part(0)
    spread_early(early_in, wide)
    for k, (table_k, p) in enumerate(((t1, p1), (t2, p2), (t3, p3))):
        first, count = LEVEL_ROWS[k]
        tiles = [wide[tile, first : first + count, :] for tile in range(4)]
        lhs = jnp.concatenate(tiles, axis=1).astype(BF16)
        p[...] = jnp.dot(lhs, table_k[0:DEEP], preferred_element_type=F32)
    products = [
        pltpu.make_async_copy(a, b, store_sem.at[5 + k])
        for k, (a, b) in enumerate(((p1, p1_out), (p2, p2_out), (p3, p3_out)))
    ]
    for copy in products:
        copy.start()
    take_part(1)
    spread_late(late_in, wide)
    done = 0
    for first, count in LEVEL_ROWS:
        rows_v[done : done + count] = wide[4, first : first + count, :].astype(BF16)
        done += count
    rows_copy = pltpu.make_async_copy(rows_v, rows_out, store_sem.at[3])
    rows_copy.start()
    for copy in products:
        copy.wait()
    for copy in tables:
        copy.wait()
    spec_copy.wait()
    rows_copy.wait()


def main_step(assign, limits, fields, legendre_t, synths):
    hbm = pl.BlockSpec(memory_space=pltpu.HBM)
    vmem = pl.BlockSpec(memory_space=pltpu.VMEM)
    smem = pl.BlockSpec(memory_space=pltpu.SMEM)
    dma = pltpu.SemaphoreType.DMA
    rows = legendre_t.shape[1]
    synths = [s.reshape(PAIR, 2, m // 2, m) for s, m in zip(synths, LEVELS)]
    wides = (1280, 640, 384)
    return pl.pallas_call(
        main_kernel,
        in_specs=[smem, smem, vmem] + [hbm] * 5,
        out_specs=[hbm] * 8,
        out_shape=[
            jax.ShapeDtypeStruct((FLD, PAIR, 2, 641), BF16),
            jax.ShapeDtypeStruct((FLD * sum(SENT), 128), BF16),
            *[jax.ShapeDtypeStruct((n, w), F32) for (_, n), w in zip(LEVEL_ROWS, wides)],
            *[jax.ShapeDtypeStruct((128, w), BF16) for w in wides],
        ],
        scratch_shapes=[
            pltpu.VMEM((PAIR, rows, 641), BF16),
            pltpu.VMEM((PAIR, NFLD * rows, 640), BF16),
            pltpu.VMEM((NFLD * rows, 128), BF16),
            pltpu.VMEM((1536, LON // 2), BF16),
            pltpu.VMEM((FLD, ROWS, LON), BF16),
            pltpu.VMEM((256, LON // 2), BF16),
            pltpu.VMEM((NLAT, 40, 1024), BF16),
            pltpu.VMEM((NLAT, 40, 1024), BF16),
            pltpu.VMEM((2, NLAT // 2, 40, 128), F32),
            pltpu.VMEM((10, 40 * FLD, 128), F32),
            pltpu.VMEM((6, 48 * PAIR, 128), F32),
            pltpu.VMEM((12, 48 * PAIR, 128), F32),
            pltpu.VMEM((512, 768), F32),
            pltpu.VMEM((FLD, PAIR, 2, 641), BF16),
            pltpu.VMEM((NLAT, 40, 384), BF16),
            pltpu.VMEM((NLAT, 40, 128), BF16),
            pltpu.VMEM((NLAT, 40, 384), BF16),
            pltpu.VMEM((NLAT, 40, 128), BF16),
            pltpu.VMEM((FLD * sum(SENT), 128), BF16),
            pltpu.VMEM((2, 640, 768), BF16),
            pltpu.VMEM((2304, 8), F32),
            pltpu.VMEM((256, 256), BF16),
            *[pltpu.VMEM(s.shape, BF16) for s in synths],
            *[pltpu.VMEM((768, w), BF16) for w in wides],
            *[pltpu.VMEM((n, w), F32) for (_, n), w in zip(LEVEL_ROWS, wides)],
            dma((PAIR,)), dma((4,)), dma((3,)), dma((8,)),
            dma((4,)), dma((4,)), dma, dma((2, 6)), dma, dma((PAIR,)),
            dma((NFLD - 1,)), dma((NFLD - 1,)), dma((2,)), dma((2,)),
        ],
        compiler_params=pltpu.CompilerParams(
            collective_id=0, has_side_effects=True, vmem_limit_bytes=64 * 1000 * 1000
        ),
    )(assign, limits, assign, fields, legendre_t, *synths)


CHUNKS = ((0, 0, 6), (0, 6, 6), (0, 12, 8), (1, 0, 10), (2, 0, 5))


def inverse_kernel(
    rows_in, spec_in, p1_in, p2_in, p3_in, t1_in, t2_in, t3_in,
    spec_out, o1_out, o2_out, o3_out,
    rows, spec, p1, p2, p3, t1, t2, t3, o1, o2, o3, in_sem, part_sem, out_sem,
):
    sums, outs = (p1, p2, p3), (o1, o2, o3)
    sources, results, tables = (p1_in, p2_in, p3_in), (o1_out, o2_out, o3_out), (t1, t2, t3)
    small = [
        pltpu.make_async_copy(a, b, in_sem.at[k])
        for k, (a, b) in enumerate(
            ((rows_in, rows), (t1_in, t1), (t2_in, t2), (t3_in, t3), (spec_in, spec))
        )
    ]
    loads, stores = [], []
    for k, (level, first, count) in enumerate(CHUNKS):
        part = pl.ds(FLD * first, FLD * count)
        loads.append(
            pltpu.make_async_copy(
                sources[level].at[part], sums[level].at[part], part_sem.at[k]
            )
        )
        part = pl.ds(first, count)
        stores.append(
            pltpu.make_async_copy(outs[level].at[part], results[level].at[part], out_sem.at[k])
        )
    for copy in small[0:2] + loads[0:3] + small[2:4] + loads[3:5] + small[4:5]:
        copy.start()
    small[0].wait()
    spec_store = pltpu.make_async_copy(spec, spec_out, out_sem.at[len(CHUNKS)])
    begin = (0, 20, 30)
    for k, (level, first, count) in enumerate(CHUNKS):
        if first == 0:
            small[1 + level].wait()
        loads[k].wait()
        start = FLD * (begin[level] + first)
        lhs = rows[start : start + FLD * count]
        z = jnp.dot(lhs, tables[level][...], preferred_element_type=F32)
        z = z + sums[level][FLD * first : FLD * (first + count)]
        size = outs[level].shape[2]
        outs[level][first : first + count] = z[:, 0:size].reshape(count, FLD, size)
        stores[k].start()
    small[4].wait()
    spec_store.start()
    for copy in stores:
        copy.wait()
    spec_store.wait()


def inverse_step(rows, spectrum, products, tables):
    shapes = [(n, FLD, 4 * m) for n, m in zip(SENT, LEVELS)]
    hbm = pl.BlockSpec(memory_space=pltpu.HBM)
    dma = pltpu.SemaphoreType.DMA
    inputs = (rows, spectrum, *products, *tables)
    return pl.pallas_call(
        inverse_kernel,
        in_specs=[hbm] * 8,
        out_specs=[hbm] * 4,
        out_shape=[jax.ShapeDtypeStruct(spectrum.shape, spectrum.dtype)]
        + [jax.ShapeDtypeStruct(s, F32) for s in shapes],
        scratch_shapes=[pltpu.VMEM(a.shape, a.dtype) for a in inputs]
        + [pltpu.VMEM(s, F32) for s in shapes]
        + [dma((5,)), dma((len(CHUNKS),)), dma((len(CHUNKS) + 1,))],
    )(*inputs)


def on_device(grid_fields, assign, limits, legendre, synth_one, synth_two, synth_three):
    spectrum, rows, *rest = main_step(
        assign,
        limits,
        grid_fields,
        jnp.transpose(legendre, (0, 2, 1)),
        (synth_one, synth_two, synth_three),
    )
    spectrum, *grids = inverse_step(rows, spectrum, rest[0:3], rest[3:6])
    return (
        jnp.transpose(spectrum, (0, 2, 1, 3)),
        *[jnp.transpose(g, (1, 0, 2)) for g in grids],
    )


def solution(mesh):
    return jax.shard_map(
        on_device,
        mesh=mesh,
        in_specs=(
            P("fld", "lat", None),
            P(),
            P(),
            P("lat", None, "fld"),
            P("lat", None, None),
            P("lat", None, None),
            P("lat", None, None),
        ),
        out_specs=(
            P("fld", None, "lat", None),
            P("fld", "lat", None),
            P("fld", "lat", None),
            P("fld", "lat", None),
        ),
        check_vma=False,
    )
```

```python
import math

import jax
import jax.numpy as jnp
from jax import lax
from jax.experimental import pallas as pl
from jax.experimental.pallas import tpu as pltpu
from jax.sharding import PartitionSpec as P

MESH = pl.DeviceIdType.MESH
F32 = jnp.float32
BF16 = jnp.bfloat16
NLAT = 32
NFLD = 4
FLD = 24
ROWS = 40
LON = 2560
PAIR = 10
SENT = (20, 10, 5)
LEVELS = (320, 160, 80)
NT = (((1,), (1,)), ((), ()))
EARLY = 8
DEEP = 2 * EARLY * NLAT


def sincos(turns):
    quarter = jnp.floor(turns * 4.0 + 0.5)
    y = (turns * 4.0 - quarter) * (math.pi / 2)
    y2 = y * y
    s = y * (1.0 + y2 * (-1.0 / 6 + y2 * (1.0 / 120 - y2 * (1.0 / 5040))))
    c = 1.0 + y2 * (-0.5 + y2 * (1.0 / 24 + y2 * (-1.0 / 720 + y2 * (1.0 / 40320))))
    k = quarter - 4.0 * jnp.floor(quarter * 0.25)
    odd = (k == 1.0) | (k == 3.0)
    sin_v = jnp.where(odd, c, s)
    cos_v = jnp.where(odd, s, c)
    sin_v = jnp.where(k >= 2.0, -sin_v, sin_v)
    cos_v = jnp.where((k == 1.0) | (k == 2.0), -cos_v, cos_v)
    return cos_v, sin_v


def turns_of(product, period):
    return (product - period * jnp.floor(product * (1.0 / period))) * (1.0 / period)


def fill_table(cols_ref, first, count, period, scale, tiles, store):
    wave = jnp.broadcast_to(cols_ref[pl.ds(first, count), 0:1], (count, 128))
    amp = jnp.broadcast_to(cols_ref[pl.ds(first, count), 1:2], (count, 128)) * scale
    comp = jnp.broadcast_to(cols_ref[pl.ds(first, count), 2:3], (count, 128))
    lane = lax.broadcasted_iota(jnp.int32, (count, 128), 1).astype(F32)
    cos_v, sin_v = sincos(turns_of(wave * lane + comp * (period // 4), float(period)))
    cos_d, sin_d = sincos(turns_of(wave * 128.0, float(period)))
    cos_v, sin_v = cos_v * amp, sin_v * amp
    for a in range(tiles):
        store(a, cos_v)
        if a + 1 < tiles:
            cos_v, sin_v = cos_v * cos_d - sin_v * sin_d, sin_v * cos_d + cos_v * sin_d


def lat_peer(k):
    return lax.rem(lax.axis_index("lat") + k, NLAT)


def greet():
    barrier = pltpu.get_barrier_semaphore()
    fld = lax.axis_index("fld")
    lat = lax.axis_index("lat")

    def one(k, carry):
        pl.semaphore_signal(barrier, inc=1, device_id=(lat_peer(k), fld), device_id_type=MESH)
        return carry

    lax.fori_loop(1, NLAT, one, 0)
    for k in range(1, NFLD):
        pl.semaphore_signal(
            barrier, inc=1, device_id=(lat, lax.rem(fld + k, NFLD)), device_id_type=MESH
        )
    return lambda: pl.semaphore_wait(barrier, NLAT + NFLD - 2)


def to_lat(src, dst, send_sem, recv_sem, k):
    return pltpu.make_async_remote_copy(
        src_ref=src,
        dst_ref=dst,
        send_sem=send_sem,
        recv_sem=recv_sem,
        device_id=(lat_peer(k), lax.axis_index("fld")),
        device_id_type=MESH,
    )


def to_fld(part, send_sem, recv_sem, k):
    fld = lax.rem(lax.axis_index("fld") + k, NFLD)
    return pltpu.make_async_remote_copy(
        src_ref=part,
        dst_ref=part,
        send_sem=send_sem,
        recv_sem=recv_sem,
        device_id=(lax.axis_index("lat"), fld),
        device_id_type=MESH,
    )


def each(first, count, act):
    def one(k, carry):
        act(k)
        return carry

    lax.fori_loop(first, count, one, 0)


def pack_pair(q, raw, main, extra, own):
    a = raw[q].astype(F32)
    t = [a[:, 128 * k : 128 * k + 128] for k in range(5)]
    last = a[:, 640:641]
    lane = lax.broadcasted_iota(jnp.int32, (a.shape[0], 128), 1)
    r = [None, None] + [pltpu.roll(t[k], 63, 1) for k in (2, 3, 4)]
    main[q, own, 0:128] = t[0].astype(BF16)
    main[q, own, 128:256] = t[1].astype(BF16)
    main[q, own, 256:384] = jnp.where(lane < 63, r[2], r[3]).astype(BF16)
    main[q, own, 384:512] = jnp.where(lane < 63, r[3], r[4]).astype(BF16)
    tail = jnp.where(lane < 127, pltpu.roll(t[4], 127, 1), last)
    main[q, own, 512:640] = jnp.where(lane < 64, t[2], tail).astype(BF16)
    column = jnp.sum(jnp.where(lane == 64, t[2], 0.0), axis=1, keepdims=True)
    extra[own] = jnp.where(lane == q, column, extra[own].astype(F32)).astype(BF16)


def dft_group(g, table, folded, perm_ref, fields, y_ref, lanes):
    x = fields[pl.ds(g * 6, 6)].astype(F32)
    low = x[:, :, : LON // 2].reshape(240, LON // 2)
    high = x[:, :, LON // 2 :].reshape(240, LON // 2)
    parts = []
    for par in range(2):
        x = low + high if par == 0 else low - high
        folded[0:120] = x[0:120].astype(BF16)
        folded[128:248] = x[120:240].astype(BF16)
        y = lax.dot_general(
            table[768 * par : 768 * par + 768], folded[...], NT, preferred_element_type=F32
        )
        y = jnp.dot(y.astype(BF16), perm_ref[...], preferred_element_type=F32)
        parts.append((y[0:512].reshape(NLAT, 16, 256), y[512:768].reshape(NLAT, 8, 256)))
    (first, mid), (last, other) = parts
    y_ref[:, :, lanes] = jnp.concatenate([first, mid + other, last], axis=1).astype(BF16)


def make_columns(assign_ref, cols, part):
    p = assign_ref[...].reshape(1, -1).astype(F32)
    total = 2.0 * assign_ref.shape[0] - 1.0
    even = jnp.where(p - 2.0 * jnp.floor(p * 0.5) > 0.5, total - p, p)
    value = (even, total - even, p)[part]
    high = jnp.floor(value * (1.0 / 16))
    place = lax.broadcasted_iota(jnp.int32, (8, value.shape[1]), 0)
    digits = jnp.where(place == 0, high, jnp.where(place == 1, value - 16.0 * high, 0.0))
    r = lax.broadcasted_iota(jnp.int32, (768, 1), 0).astype(F32)
    if part < 2:
        rest = r >= 512.0
        s = jnp.where(rest, r - 512.0, r)
        l = jnp.where(rest, jnp.floor((s + 0.5) * (1.0 / 8)), jnp.floor((s + 0.5) * (1.0 / 16)))
        i = s - jnp.where(rest, 8.0, 16.0) * l
        if part == 0:
            valid = jnp.logical_not(rest) | (i < 4.0)
            q = jnp.floor(i * 0.5) + jnp.where(rest, 8.0, 0.0)
        else:
            valid = jnp.logical_not(rest) | (i >= 4.0)
            q = jnp.floor(i * 0.5) + jnp.where(rest, 6.0, 0.0)
    else:
        late = r >= 512.0
        s = jnp.where(late, r - 512.0, r)
        valid = r < 640.0
        high_part = jnp.floor((s + 0.5) * jnp.where(late, 1.0 / 32, 1.0 / 16))
        low_part = s - jnp.where(late, 32.0, 16.0) * high_part
        l = jnp.where(late, low_part, high_part)
        i = jnp.where(late, high_part, low_part)
        q = jnp.floor(i * 0.5) + jnp.where(late, 8.0, 0.0)
    slot = jnp.where(valid, 10.0 * l + q, -1.0)
    lane = lax.broadcasted_iota(jnp.int32, (768, value.shape[1]), 1).astype(F32)
    picker = jnp.where(lane == slot, 1.0, 0.0).astype(BF16)
    found = lax.dot_general(picker, digits.astype(BF16), NT, preferred_element_type=F32)
    wave = 16.0 * found[:, 0:1] + found[:, 1:2]
    amp = jnp.where(valid, 1.0, 0.0)
    if part == 2:
        amp = amp * jnp.where(wave > 0.5, 2.0, 1.0)
    rows = slice(768 * part, 768 * part + 768)
    cols[rows, 0:1] = wave
    cols[rows, 1:2] = amp
    cols[rows, 2:3] = i - 2.0 * jnp.floor(i * 0.5)


def make_turner(perm):
    u = lax.broadcasted_iota(jnp.int32, (256, 256), 0).astype(F32)
    v = lax.broadcasted_iota(jnp.int32, (256, 256), 1).astype(F32)
    inner = v - 128.0 * jnp.floor(v * (1.0 / 128))
    t = inner - 40.0 * jnp.floor((inner + 0.5) * (1.0 / 40))
    source = jnp.where(lax.axis_index("lat") >= NLAT // 2, v + 39.0 - 2.0 * t, v)
    perm[...] = jnp.where((u == source) & (inner < 120.0), 1.0, 0.0).astype(BF16)


def gather_lanes(pieces, width, offset, tile, lane):
    first, last = 128 * tile // width, min((128 * tile + 127) // width, len(pieces) - 1)
    total = None
    for l in range(first, last + 1):
        turned = pltpu.roll(pieces[l](), (width * l - offset) % 128, 1)
        start = width * l - 128 * tile
        total = turned if total is None else jnp.where(lane >= start, turned, total)
    return total


def strided(ref, lead, tiles, first, count, step):
    parts = [ref[lead + k, pl.ds(first, count, stride=step), :] for k in range(tiles)]
    return jnp.concatenate(parts, axis=1)


def fold_fields(ft, x_ref, folded, wide):
    half = NLAT // 2
    lane = lax.broadcasted_iota(jnp.int32, (40, 128), 1)
    lanes = pl.ds(pl.multiple_of(ft * 128, 128), 128)
    for l in range(half):
        n = x_ref[l, :, lanes].astype(F32)
        s = x_ref[NLAT - 1 - l, :, lanes].astype(F32)
        folded[0, l] = n + s
        folded[1, l] = n - s
    for sign in range(2):
        pieces = [lambda l=l: folded[sign, l] for l in range(half)]
        for tile in range(5):
            for fi in range(3):
                value = gather_lanes(pieces, ROWS, ROWS * fi, tile, lane)
                first = pl.multiple_of((3 * ft + fi) * 40, 8)
                wide[5 * sign + tile, pl.ds(first, 40), :] = value


def legendre_pair(q, p, limits, wide, main, extra, synths, joined, levels):
    def operand(sign):
        parts = []
        for par in range(2):
            for c in range(2):
                row = 2 * q + c
                if par == 1:
                    row += 24 - 20 * lax.div(q, 8)
                parts.append(strided(wide, 5 * sign, 5, row, FLD, 40))
        return jnp.concatenate(parts, axis=0).astype(BF16)

    sym, anti = operand(0), operand(1)
    lane96 = lax.broadcasted_iota(jnp.int32, (96, 128), 1)
    z_sym = jnp.dot(sym, main[q, :, 0:256], preferred_element_type=F32)
    z_anti = jnp.dot(anti, main[q, :, 256:512], preferred_element_type=F32)
    tail = main[q, :, 512:640]
    z_tail = jnp.where(
        lane96 < 64,
        jnp.dot(sym, tail, preferred_element_type=F32),
        jnp.dot(anti, tail, preferred_element_type=F32),
    )
    z_extra = jnp.dot(sym, extra[...], preferred_element_type=F32)
    z_extra = jnp.sum(jnp.where(lane96 == q, z_extra, 0.0), axis=1, keepdims=True)
    first_sym = lax.shift_right_logical(641 - p, 1)
    first_anti = lax.shift_right_logical(640 - p, 1)
    parity = lax.bitwise_and(p, 1)

    def choose(z, rank, first):
        taken = jnp.where(rank < first, 1, 0) ^ parity
        return jnp.where(taken == 1, z[0:48], z[48:96])

    lane = lax.broadcasted_iota(jnp.int32, (48, 128), 1)
    rank = lax.broadcasted_iota(jnp.int32, (48, 256), 1)
    z_sym = choose(z_sym, rank, first_sym).astype(BF16)
    z_anti = choose(z_anti, rank, first_anti).astype(BF16)
    z_tail = jnp.where(
        lane < 64,
        choose(z_tail, lane + 256, first_sym),
        choose(z_tail, lane + 192, first_anti),
    )
    z_tail = z_tail.astype(BF16).astype(F32)
    z_extra = choose(jnp.broadcast_to(z_extra, (96, 128)), lane * 0 + 320, first_sym)
    sym32, anti32 = z_sym.astype(F32), z_anti.astype(F32)
    low, high = pltpu.roll(anti32[:, 0:128], 65, 1), pltpu.roll(anti32[:, 128:256], 65, 1)
    end = pltpu.roll(z_tail, 1, 1)
    own = pl.ds(pl.multiple_of(q * 48, 48), 48)
    joined[0, own] = sym32[:, 0:128]
    joined[1, own] = sym32[:, 128:256]
    joined[2, own] = jnp.where(lane < 64, z_tail, jnp.where(lane == 64, z_extra, low))
    joined[3, own] = jnp.where(lane < 65, low, high)
    joined[4, own] = jnp.where(lane < 65, high, end)
    joined[5, own] = end

    for level, place in enumerate((0, 3, 5)):
        size = LEVELS[level]
        h = size // 2
        degree = p + 2 * rank
        kept_sym = jnp.where(degree <= limits[level], sym32, 0.0).astype(BF16)[:, 0:h]
        kept_anti = jnp.where(degree + 1 <= limits[level], anti32, 0.0).astype(BF16)[:, 0:h]
        even = jnp.dot(kept_sym, synths[level][q, 0], preferred_element_type=F32)
        odd = jnp.dot(kept_anti, synths[level][q, 1], preferred_element_type=F32)
        for sign, value in enumerate((even + odd, even - odd)):
            for k in range(0, size, 128):
                width = min(128, size - k)
                levels[6 * sign + place + k // 128, own, 0:width] = value[:, k : k + width]


def make_pickers(pickers):
    row = lax.broadcasted_iota(jnp.int32, (640, 1), 0).astype(F32)
    lane_of = lax.broadcasted_iota(jnp.int32, (640, 768), 1).astype(F32)
    block = jnp.floor((row + 0.5) * (1.0 / 40))
    t = row - 40.0 * block
    for sign in range(2):
        at = [t, t - 24.0, t - 34.0]
        if sign == 1:
            at = [19.0 - t, 33.0 - t, 38.0 - t]
        target = jnp.where(
            t < 20.0,
            20.0 * block + at[0],
            jnp.where(
                (t >= 24.0) & (t < 34.0),
                384.0 + 10.0 * block + at[1],
                jnp.where((t >= 34.0) & (t < 39.0), 640.0 + 5.0 * block + at[2], -1.0),
            ),
        )
        pickers[sign] = jnp.where(lane_of == target, 1.0, 0.0).astype(BF16)


def turn_levels(part, levels, turned, pickers, blocks):
    half = NLAT // 2
    base = 0 if part == 0 else 2 * EARLY * FLD
    size = blocks.shape[2]
    for sign in range(2):
        if part == 0:
            for f in range(FLD):
                value = strided(levels, 6 * sign, 6, f, 2 * EARLY, FLD)
                turned[2 * EARLY * f : 2 * EARLY * (f + 1)] = value
        else:
            for i in range(2 * (PAIR - EARLY)):
                first = base + FLD * i
                tiles = [levels[6 * sign + k, first : first + FLD, :] for k in range(6)]
                first = base + 32 * i
                turned[first : first + FLD] = jnp.concatenate(tiles, axis=1)
        picked = lax.dot_general(
            pickers[sign],
            turned[base : base + size].astype(BF16),
            NT,
            preferred_element_type=F32,
        )
        picked = picked.reshape(half, 40, size).astype(BF16)
        if sign == 0:
            blocks[0:half] = picked
        else:
            for m in range(half):
                blocks[NLAT - 1 - m] = picked[m]


def swap_units(values, width):
    lane = lax.broadcasted_iota(jnp.int32, values[0].shape, 1)
    values = list(values)
    k = 1
    while k < len(values):
        upper = (lane & (k * width)) != 0
        for a in range(len(values)):
            if a & k == 0:
                low, high = values[a], values[a + k]
                values[a] = jnp.where(upper, pltpu.roll(high, k * width, 1), low)
                values[a + k] = jnp.where(upper, high, pltpu.roll(low, 128 - k * width, 1))
        k *= 2
    return values


def spread_early(arrived, wide):
    def group(g):
        lanes = pl.ds(pl.multiple_of(g * 128, 128), 128)
        for tile in range(4):
            values = [arrived[8 * tile + a, :, lanes].astype(F32) for a in range(8)]
            for a, value in enumerate(swap_units(values, 16)):
                wide[tile, pl.ds(8 * g + a, 40, stride=FLD), :] = value

    each(0, 3, group)


def spread_late(arrived, wide):
    def rows(b):
        own = pl.ds(pl.multiple_of(8 * b, 8), 8)
        values = [arrived[l, own, :].astype(F32) for l in range(NLAT)]
        for f, value in enumerate(swap_units(values, 1)[0:FLD]):
            wide[4, pl.ds(8 * FLD * b + f, 8, stride=FLD), :] = value

    each(0, 5, rows)


LEVEL_ROWS = ((0, 480), (576, 240), (816, 120))


def main_kernel(
    assign_s, limits, assign_v, fields_in, legendre_in, s1_in, s2_in, s3_in,
    spec_out, rows_out, p1_out, p2_out, p3_out, t1_out, t2_out, t3_out,
    raw, main, extra, table, fields, folded_rows, y, x, folded, wide, joined, levels, turned,
    spec, early, late, early_in, late_in, rows_v, pickers, cols, perm, s1, s2, s3, t1, t2, t3,
    p1, p2, p3,
    raw_sem, field_sem, load_sem, store_sem, y_send, y_recv, near_send, near_recv,
    far_send, far_recv, extra_send, extra_recv, block_send, block_recv,
):
    lat = lax.axis_index("lat")
    fld = lax.axis_index("fld")
    rows = legendre_in.shape[1]
    own = pl.ds(pl.multiple_of(fld * rows, rows), rows)
    synths = (s1, s2, s3)

    def raw_copy(q):
        return pltpu.make_async_copy(legendre_in.at[q], raw.at[q], raw_sem.at[q])

    def field_copy(g):
        part = pl.ds(g * 6, 6)
        return pltpu.make_async_copy(fields_in.at[part], fields.at[part], field_sem.at[g])

    loads = [
        pltpu.make_async_copy(a, b, load_sem.at[k])
        for k, (a, b) in enumerate(((s1_in, s1), (s2_in, s2), (s3_in, s3)))
    ]
    tables = [
        pltpu.make_async_copy(a.at[pl.ds(DEEP, 128)], b, store_sem.at[k])
        for k, (a, b) in enumerate(((t1, t1_out), (t2, t2_out), (t3, t3_out)))
    ]
    each(0, PAIR, lambda q: raw_copy(q).start())
    all_greeted = greet()
    each(0, 4, lambda g: field_copy(g).start())
    for copy in loads:
        copy.start()
    extra[own] = jnp.zeros((rows, 128), BF16)

    def shard(q, k):
        s = lax.rem(fld + k, NFLD)
        return main.at[q, pl.ds(pl.multiple_of(s * rows, rows), rows)]

    def near(h, way):
        pair = main.at[pl.ds(2 * h, 2), own]
        return to_fld(pair, near_send, near_recv.at[way, h], 1 + 2 * way)

    def near_last(q, way):
        return to_fld(shard(q, 0), near_send, near_recv.at[way, q - 4], 1 + 2 * way)

    def far(q, way):
        return to_fld(shard(q, 3 - 2 * way), far_send, far_recv.at[q], 1 + 2 * way)

    def extra_copy(k):
        return to_fld(extra.at[own], extra_send.at[k - 1], extra_recv.at[k - 1], k)

    def start_near(h):
        near(h, 0).start()
        near(h, 1).start()

    def start_last():
        near_last(8, 0).start()
        near_last(9, 1).start()
        near_last(9, 0).start()
        near_last(8, 1).start()

    def pack_one(q):
        raw_copy(q).wait()
        pack_pair(q, raw, main, extra, own)

    pack_one(0)
    pack_one(1)
    all_greeted()
    start_near(0)
    pack_one(2)
    pack_one(3)
    folded_rows[...] = jnp.zeros_like(folded_rows)
    make_columns(assign_v, cols, 0)
    make_columns(assign_v, cols, 1)
    make_turner(perm)

    def fill(b):
        first = pl.multiple_of(b * 64, 64)

        def store(a, value):
            table[pl.ds(first, 64), 128 * a : 128 * a + 128] = value.astype(BF16)

        fill_table(cols, first, 64, LON, 1.0 / math.sqrt(LON), 10, store)

    each(0, 24, fill)
    start_near(1)

    def lanes_of(g):
        return pl.ds(pl.multiple_of(g * 256, 256), 256)

    def y_copy(g, k):
        return to_lat(
            y.at[lat_peer(k), :, lanes_of(g)],
            x.at[lat, :, lanes_of(g)],
            y_send.at[g],
            y_recv.at[g],
            k,
        )

    def y_wait(g):
        part = pl.ds(0, NLAT - 1)
        both = to_lat(
            y.at[part, :, lanes_of(g)], x.at[part, :, lanes_of(g)], y_send.at[g], y_recv.at[g], 1
        )
        both.wait_send()
        both.wait_recv()

    def relay(h):
        near(h, 0).wait_recv()
        far(2 * h, 0).start()
        near(h, 1).wait_recv()
        far(2 * h + 1, 1).start()

    def transform(g):
        field_copy(g).wait()
        dft_group(g, table, folded_rows, perm, fields, y, lanes_of(g))
        x[lat, :, lanes_of(g)] = y[lat, :, lanes_of(g)]

    def send_group(g):
        each(1, NLAT, lambda k: y_copy(g, k).start())

    def group(g):
        transform(g)
        pack_one(2 * g + 4)
        pack_one(2 * g + 5)
        send_group(g)

        @pl.when(g < 2)
        def _():
            start_near(g + 2)

        @pl.when(g > 0)
        def _():
            relay(g - 1)

    each(0, 3, group)
    transform(3)
    send_group(3)
    for k in range(1, NFLD):
        extra_copy(k).start()

    levels[...] = jnp.zeros_like(levels)
    turned[...] = jnp.zeros_like(turned)
    make_pickers(pickers)
    make_columns(assign_v, cols, 2)

    def fill_inverse(b):
        first = pl.multiple_of(b * 64, 64)
        for out, size, tiles in ((t1, 1280, 10), (t2, 640, 5), (t3, 320, 3)):

            def store(a, value, out=out):
                out[pl.ds(first, 64), 128 * a : 128 * a + 128] = value.astype(BF16)

            fill_table(cols, 1536 + first, 64, size, 1.0 / math.sqrt(size), tiles, store)

    each(0, 12, fill_inverse)
    for copy in tables:
        copy.start()

    def take_group(g):
        y_wait(g)
        fold_fields(2 * g, x, folded, wide)
        fold_fields(2 * g + 1, x, folded, wide)

        @pl.when(g == 0)
        def _():
            relay(2)

        @pl.when(g == 2)
        def _():
            relay(3)
            start_last()

    each(0, 4, take_group)
    for copy in loads:
        copy.wait()
    for k in range(1, NFLD):
        extra_copy(k).wait()

    parts = ((early, early_in), (late, late_in))

    def block_copy(part, k):
        return to_lat(
            parts[part][0].at[lat_peer(k)],
            parts[part][1].at[lat],
            block_send.at[part],
            block_recv.at[part],
            k,
        )

    def pair(q):
        way = lax.rem(q, 2)
        far(q, way).wait_recv()
        p = assign_s[PAIR * lat + q]
        legendre_pair(q, p, limits, wide, main, extra, synths, joined, levels)

    def send_part(part):
        turn_levels(part, levels, turned, pickers, parts[part][0])
        parts[part][1][lat] = parts[part][0][lat]
        each(1, NLAT, lambda k: block_copy(part, k).start())

    def take_part(part):
        count = pl.ds(0, NLAT - 1)
        both = to_lat(
            parts[part][0].at[count], parts[part][1].at[count], block_send.at[part],
            block_recv.at[part], 1,
        )
        both.wait_send()
        both.wait_recv()

    each(0, EARLY, pair)
    send_part(0)
    near_last(8, 0).wait_recv()
    far(8, 0).start()
    near_last(9, 1).wait_recv()
    far(9, 1).start()
    near_last(8, 1).wait_recv()
    near_last(9, 0).wait_recv()
    each(EARLY, PAIR, pair)
    send_part(1)

    def field(f):
        part = strided(joined, 0, 6, f, 2 * PAIR, FLD)
        spec[f] = part[:, 0:641].reshape(PAIR, 2, 641).astype(BF16)

    each(0, FLD, field)
    spec_copy = pltpu.make_async_copy(spec, spec_out, store_sem.at[4])
    spec_copy.start()

    first_two = main.at[:, pl.ds(0, 2 * rows)]
    to_fld(first_two, near_send, near_recv.at[0, 0], 1).wait_send()
    to_fld(main.at[:, pl.ds(0, rows)], far_send, far_recv.at[0], 1).wait_send()
    take_part(0)
    spread_early(early_in, wide)
    for k, (table_k, p) in enumerate(((t1, p1), (t2, p2), (t3, p3))):
        first, count = LEVEL_ROWS[k]
        tiles = [wide[tile, first : first + count, :] for tile in range(4)]
        lhs = jnp.concatenate(tiles, axis=1).astype(BF16)
        p[...] = jnp.dot(lhs, table_k[0:DEEP], preferred_element_type=F32)
    products = [
        pltpu.make_async_copy(a, b, store_sem.at[5 + k])
        for k, (a, b) in enumerate(((p1, p1_out), (p2, p2_out), (p3, p3_out)))
    ]
    for copy in products:
        copy.start()
    take_part(1)
    spread_late(late_in, wide)
    done = 0
    for first, count in LEVEL_ROWS:
        rows_v[done : done + count] = wide[4, first : first + count, :].astype(BF16)
        done += count
    rows_copy = pltpu.make_async_copy(rows_v, rows_out, store_sem.at[3])
    rows_copy.start()
    for copy in products:
        copy.wait()
    for copy in tables:
        copy.wait()
    spec_copy.wait()
    rows_copy.wait()


def main_step(assign, limits, fields, legendre_t, synths):
    hbm = pl.BlockSpec(memory_space=pltpu.HBM)
    vmem = pl.BlockSpec(memory_space=pltpu.VMEM)
    smem = pl.BlockSpec(memory_space=pltpu.SMEM)
    dma = pltpu.SemaphoreType.DMA
    rows = legendre_t.shape[1]
    synths = [s.reshape(PAIR, 2, m // 2, m) for s, m in zip(synths, LEVELS)]
    wides = (1280, 640, 384)
    return pl.pallas_call(
        main_kernel,
        in_specs=[smem, smem, vmem] + [hbm] * 5,
        out_specs=[hbm] * 8,
        out_shape=[
            jax.ShapeDtypeStruct((FLD, PAIR, 2, 641), BF16),
            jax.ShapeDtypeStruct((FLD * sum(SENT), 128), BF16),
            *[jax.ShapeDtypeStruct((n, w), F32) for (_, n), w in zip(LEVEL_ROWS, wides)],
            *[jax.ShapeDtypeStruct((128, w), BF16) for w in wides],
        ],
        scratch_shapes=[
            pltpu.VMEM((PAIR, rows, 641), BF16),
            pltpu.VMEM((PAIR, NFLD * rows, 640), BF16),
            pltpu.VMEM((NFLD * rows, 128), BF16),
            pltpu.VMEM((1536, LON // 2), BF16),
            pltpu.VMEM((FLD, ROWS, LON), BF16),
            pltpu.VMEM((256, LON // 2), BF16),
            pltpu.VMEM((NLAT, 40, 1024), BF16),
            pltpu.VMEM((NLAT, 40, 1024), BF16),
            pltpu.VMEM((2, NLAT // 2, 40, 128), F32),
            pltpu.VMEM((10, 40 * FLD, 128), F32),
            pltpu.VMEM((6, 48 * PAIR, 128), F32),
            pltpu.VMEM((12, 48 * PAIR, 128), F32),
            pltpu.VMEM((512, 768), F32),
            pltpu.VMEM((FLD, PAIR, 2, 641), BF16),
            pltpu.VMEM((NLAT, 40, 384), BF16),
            pltpu.VMEM((NLAT, 40, 128), BF16),
            pltpu.VMEM((NLAT, 40, 384), BF16),
            pltpu.VMEM((NLAT, 40, 128), BF16),
            pltpu.VMEM((FLD * sum(SENT), 128), BF16),
            pltpu.VMEM((2, 640, 768), BF16),
            pltpu.VMEM((2304, 8), F32),
            pltpu.VMEM((256, 256), BF16),
            *[pltpu.VMEM(s.shape, BF16) for s in synths],
            *[pltpu.VMEM((768, w), BF16) for w in wides],
            *[pltpu.VMEM((n, w), F32) for (_, n), w in zip(LEVEL_ROWS, wides)],
            dma((PAIR,)), dma((4,)), dma((3,)), dma((8,)),
            dma((4,)), dma((4,)), dma, dma((2, 6)), dma, dma((PAIR,)),
            dma((NFLD - 1,)), dma((NFLD - 1,)), dma((2,)), dma((2,)),
        ],
        compiler_params=pltpu.CompilerParams(
            collective_id=0, has_side_effects=True, vmem_limit_bytes=64 * 1000 * 1000
        ),
    )(assign, limits, assign, fields, legendre_t, *synths)


CHUNKS = ((0, 0, 6), (0, 6, 6), (0, 12, 8), (1, 0, 10), (2, 0, 5))


def inverse_kernel(
    rows_in, spec_in, p1_in, p2_in, p3_in, t1_in, t2_in, t3_in,
    spec_out, o1_out, o2_out, o3_out,
    rows, spec, p1, p2, p3, t1, t2, t3, o1, o2, o3, in_sem, part_sem, out_sem,
):
    sums, outs = (p1, p2, p3), (o1, o2, o3)
    sources, results, tables = (p1_in, p2_in, p3_in), (o1_out, o2_out, o3_out), (t1, t2, t3)
    small = [
        pltpu.make_async_copy(a, b, in_sem.at[k])
        for k, (a, b) in enumerate(
            ((rows_in, rows), (t1_in, t1), (t2_in, t2), (t3_in, t3), (spec_in, spec))
        )
    ]
    loads, stores = [], []
    for k, (level, first, count) in enumerate(CHUNKS):
        part = pl.ds(FLD * first, FLD * count)
        loads.append(
            pltpu.make_async_copy(
                sources[level].at[part], sums[level].at[part], part_sem.at[k]
            )
        )
        part = pl.ds(first, count)
        stores.append(
            pltpu.make_async_copy(outs[level].at[part], results[level].at[part], out_sem.at[k])
        )
    for copy in small[0:2] + loads[0:3] + small[2:4] + loads[3:5] + small[4:5]:
        copy.start()
    small[0].wait()
    spec_store = pltpu.make_async_copy(spec, spec_out, out_sem.at[len(CHUNKS)])
    begin = (0, 20, 30)
    for k, (level, first, count) in enumerate(CHUNKS):
        if first == 0:
            small[1 + level].wait()
        loads[k].wait()
        start = FLD * (begin[level] + first)
        lhs = rows[start : start + FLD * count]
        z = jnp.dot(lhs, tables[level][...], preferred_element_type=F32)
        z = z + sums[level][FLD * first : FLD * (first + count)]
        size = outs[level].shape[2]
        outs[level][first : first + count] = z[:, 0:size].reshape(count, FLD, size)
        stores[k].start()
    small[4].wait()
    spec_store.start()
    for copy in stores:
        copy.wait()
    spec_store.wait()


def inverse_step(rows, spectrum, products, tables):
    shapes = [(n, FLD, 4 * m) for n, m in zip(SENT, LEVELS)]
    hbm = pl.BlockSpec(memory_space=pltpu.HBM)
    dma = pltpu.SemaphoreType.DMA
    inputs = (rows, spectrum, *products, *tables)
    return pl.pallas_call(
        inverse_kernel,
        in_specs=[hbm] * 8,
        out_specs=[hbm] * 4,
        out_shape=[jax.ShapeDtypeStruct(spectrum.shape, spectrum.dtype)]
        + [jax.ShapeDtypeStruct(s, F32) for s in shapes],
        scratch_shapes=[pltpu.VMEM(a.shape, a.dtype) for a in inputs]
        + [pltpu.VMEM(s, F32) for s in shapes]
        + [dma((5,)), dma((len(CHUNKS),)), dma((len(CHUNKS) + 1,))],
    )(*inputs)


def on_device(grid_fields, assign, limits, legendre, synth_one, synth_two, synth_three):
    spectrum, rows, *rest = main_step(
        assign,
        limits,
        grid_fields,
        jnp.transpose(legendre, (0, 2, 1)),
        (synth_one, synth_two, synth_three),
    )
    spectrum, *grids = inverse_step(rows, spectrum, rest[0:3], rest[3:6])
    return (
        jnp.transpose(spectrum, (0, 2, 1, 3)),
        *[jnp.transpose(g, (1, 0, 2)) for g in grids],
    )


def solution(mesh):
    return jax.shard_map(
        on_device,
        mesh=mesh,
        in_specs=(
            P("fld", "lat", None),
            P(),
            P(),
            P("lat", None, "fld"),
            P("lat", None, None),
            P("lat", None, None),
            P("lat", None, None),
        ),
        out_specs=(
            P("fld", None, "lat", None),
            P("fld", "lat", None),
            P("fld", "lat", None),
            P("fld", "lat", None),
        ),
        check_vma=False,
    )
```

```python
import math

import jax
import jax.numpy as jnp
from jax import lax
from jax.experimental import pallas as pl
from jax.experimental.pallas import tpu as pltpu
from jax.sharding import PartitionSpec as P

MESH = pl.DeviceIdType.MESH
F32 = jnp.float32
BF16 = jnp.bfloat16
NLAT = 32
NFLD = 4
FLD = 24
ROWS = 40
LON = 2560
PAIR = 10
SENT = (20, 10, 5)
LEVELS = (320, 160, 80)
NT = (((1,), (1,)), ((), ()))
EARLY = 8
DEEP = 2 * EARLY * NLAT


def sincos(turns):
    quarter = jnp.floor(turns * 4.0 + 0.5)
    y = (turns * 4.0 - quarter) * (math.pi / 2)
    y2 = y * y
    s = y * (1.0 + y2 * (-1.0 / 6 + y2 * (1.0 / 120 - y2 * (1.0 / 5040))))
    c = 1.0 + y2 * (-0.5 + y2 * (1.0 / 24 + y2 * (-1.0 / 720 + y2 * (1.0 / 40320))))
    k = quarter - 4.0 * jnp.floor(quarter * 0.25)
    odd = (k == 1.0) | (k == 3.0)
    sin_v = jnp.where(odd, c, s)
    cos_v = jnp.where(odd, s, c)
    sin_v = jnp.where(k >= 2.0, -sin_v, sin_v)
    cos_v = jnp.where((k == 1.0) | (k == 2.0), -cos_v, cos_v)
    return cos_v, sin_v


def turns_of(product, period):
    return (product - period * jnp.floor(product * (1.0 / period))) * (1.0 / period)


def fill_table(cols_ref, first, count, period, scale, tiles, store):
    wave = jnp.broadcast_to(cols_ref[pl.ds(first, count), 0:1], (count, 128))
    amp = jnp.broadcast_to(cols_ref[pl.ds(first, count), 1:2], (count, 128)) * scale
    comp = jnp.broadcast_to(cols_ref[pl.ds(first, count), 2:3], (count, 128))
    lane = lax.broadcasted_iota(jnp.int32, (count, 128), 1).astype(F32)
    cos_v, sin_v = sincos(turns_of(wave * lane + comp * (period // 4), float(period)))
    cos_d, sin_d = sincos(turns_of(wave * 128.0, float(period)))
    cos_v, sin_v = cos_v * amp, sin_v * amp
    for a in range(tiles):
        store(a, cos_v)
        if a + 1 < tiles:
            cos_v, sin_v = cos_v * cos_d - sin_v * sin_d, sin_v * cos_d + cos_v * sin_d


def lat_peer(k):
    return lax.rem(lax.axis_index("lat") + k, NLAT)


def greet():
    barrier = pltpu.get_barrier_semaphore()
    fld = lax.axis_index("fld")
    lat = lax.axis_index("lat")

    def one(k, carry):
        pl.semaphore_signal(barrier, inc=1, device_id=(lat_peer(k), fld), device_id_type=MESH)
        return carry

    lax.fori_loop(1, NLAT, one, 0)
    for k in range(1, NFLD):
        pl.semaphore_signal(
            barrier, inc=1, device_id=(lat, lax.rem(fld + k, NFLD)), device_id_type=MESH
        )
    return lambda: pl.semaphore_wait(barrier, NLAT + NFLD - 2)


def to_lat(src, dst, send_sem, recv_sem, k):
    return pltpu.make_async_remote_copy(
        src_ref=src,
        dst_ref=dst,
        send_sem=send_sem,
        recv_sem=recv_sem,
        device_id=(lat_peer(k), lax.axis_index("fld")),
        device_id_type=MESH,
    )


def to_fld(part, send_sem, recv_sem, k):
    fld = lax.rem(lax.axis_index("fld") + k, NFLD)
    return pltpu.make_async_remote_copy(
        src_ref=part,
        dst_ref=part,
        send_sem=send_sem,
        recv_sem=recv_sem,
        device_id=(lax.axis_index("lat"), fld),
        device_id_type=MESH,
    )


def each(first, count, act):
    def one(k, carry):
        act(k)
        return carry

    lax.fori_loop(first, count, one, 0)


def pack_pair(q, raw, main, extra, own):
    a = raw[q].astype(F32)
    t = [a[:, 128 * k : 128 * k + 128] for k in range(5)]
    last = a[:, 640:641]
    lane = lax.broadcasted_iota(jnp.int32, (a.shape[0], 128), 1)
    r = [None, None] + [pltpu.roll(t[k], 63, 1) for k in (2, 3, 4)]
    main[q, own, 0:128] = t[0].astype(BF16)
    main[q, own, 128:256] = t[1].astype(BF16)
    main[q, own, 256:384] = jnp.where(lane < 63, r[2], r[3]).astype(BF16)
    main[q, own, 384:512] = jnp.where(lane < 63, r[3], r[4]).astype(BF16)
    tail = jnp.where(lane < 127, pltpu.roll(t[4], 127, 1), last)
    main[q, own, 512:640] = jnp.where(lane < 64, t[2], tail).astype(BF16)
    column = jnp.sum(jnp.where(lane == 64, t[2], 0.0), axis=1, keepdims=True)
    extra[own] = jnp.where(lane == q, column, extra[own].astype(F32)).astype(BF16)


def dft_group(g, table, folded, perm_ref, fields, y_ref, lanes):
    x = fields[pl.ds(g * 6, 6)].astype(F32)
    low = x[:, :, : LON // 2].reshape(240, LON // 2)
    high = x[:, :, LON // 2 :].reshape(240, LON // 2)
    parts = []
    for par in range(2):
        x = low + high if par == 0 else low - high
        folded[0:120] = x[0:120].astype(BF16)
        folded[128:248] = x[120:240].astype(BF16)
        y = lax.dot_general(
            table[768 * par : 768 * par + 768], folded[...], NT, preferred_element_type=F32
        )
        y = jnp.dot(y.astype(BF16), perm_ref[...], preferred_element_type=F32)
        parts.append((y[0:512].reshape(NLAT, 16, 256), y[512:768].reshape(NLAT, 8, 256)))
    (first, mid), (last, other) = parts
    y_ref[:, :, lanes] = jnp.concatenate([first, mid + other, last], axis=1).astype(BF16)


def make_columns(assign_ref, cols, part):
    p = assign_ref[...].reshape(1, -1).astype(F32)
    total = 2.0 * assign_ref.shape[0] - 1.0
    even = jnp.where(p - 2.0 * jnp.floor(p * 0.5) > 0.5, total - p, p)
    value = (even, total - even, p)[part]
    high = jnp.floor(value * (1.0 / 16))
    place = lax.broadcasted_iota(jnp.int32, (8, value.shape[1]), 0)
    digits = jnp.where(place == 0, high, jnp.where(place == 1, value - 16.0 * high, 0.0))
    r = lax.broadcasted_iota(jnp.int32, (768, 1), 0).astype(F32)
    if part < 2:
        rest = r >= 512.0
        s = jnp.where(rest, r - 512.0, r)
        l = jnp.where(rest, jnp.floor((s + 0.5) * (1.0 / 8)), jnp.floor((s + 0.5) * (1.0 / 16)))
        i = s - jnp.where(rest, 8.0, 16.0) * l
        if part == 0:
            valid = jnp.logical_not(rest) | (i < 4.0)
            q = jnp.floor(i * 0.5) + jnp.where(rest, 8.0, 0.0)
        else:
            valid = jnp.logical_not(rest) | (i >= 4.0)
            q = jnp.floor(i * 0.5) + jnp.where(rest, 6.0, 0.0)
    else:
        late = r >= 512.0
        s = jnp.where(late, r - 512.0, r)
        valid = r < 640.0
        high_part = jnp.floor((s + 0.5) * jnp.where(late, 1.0 / 32, 1.0 / 16))
        low_part = s - jnp.where(late, 32.0, 16.0) * high_part
        l = jnp.where(late, low_part, high_part)
        i = jnp.where(late, high_part, low_part)
        q = jnp.floor(i * 0.5) + jnp.where(late, 8.0, 0.0)
    slot = jnp.where(valid, 10.0 * l + q, -1.0)
    lane = lax.broadcasted_iota(jnp.int32, (768, value.shape[1]), 1).astype(F32)
    picker = jnp.where(lane == slot, 1.0, 0.0).astype(BF16)
    found = lax.dot_general(picker, digits.astype(BF16), NT, preferred_element_type=F32)
    wave = 16.0 * found[:, 0:1] + found[:, 1:2]
    amp = jnp.where(valid, 1.0, 0.0)
    if part == 2:
        amp = amp * jnp.where(wave > 0.5, 2.0, 1.0)
    rows = slice(768 * part, 768 * part + 768)
    cols[rows, 0:1] = wave
    cols[rows, 1:2] = amp
    cols[rows, 2:3] = i - 2.0 * jnp.floor(i * 0.5)


def make_turner(perm):
    u = lax.broadcasted_iota(jnp.int32, (256, 256), 0).astype(F32)
    v = lax.broadcasted_iota(jnp.int32, (256, 256), 1).astype(F32)
    inner = v - 128.0 * jnp.floor(v * (1.0 / 128))
    t = inner - 40.0 * jnp.floor((inner + 0.5) * (1.0 / 40))
    source = jnp.where(lax.axis_index("lat") >= NLAT // 2, v + 39.0 - 2.0 * t, v)
    perm[...] = jnp.where((u == source) & (inner < 120.0), 1.0, 0.0).astype(BF16)


def gather_lanes(pieces, width, offset, tile, lane):
    first, last = 128 * tile // width, min((128 * tile + 127) // width, len(pieces) - 1)
    total = None
    for l in range(first, last + 1):
        turned = pltpu.roll(pieces[l](), (width * l - offset) % 128, 1)
        start = width * l - 128 * tile
        total = turned if total is None else jnp.where(lane >= start, turned, total)
    return total


def strided(ref, lead, tiles, first, count, step):
    parts = [ref[lead + k, pl.ds(first, count, stride=step), :] for k in range(tiles)]
    return jnp.concatenate(parts, axis=1)


def fold_fields(ft, x_ref, folded, wide):
    half = NLAT // 2
    lane = lax.broadcasted_iota(jnp.int32, (40, 128), 1)
    lanes = pl.ds(pl.multiple_of(ft * 128, 128), 128)
    for l in range(half):
        n = x_ref[l, :, lanes].astype(F32)
        s = x_ref[NLAT - 1 - l, :, lanes].astype(F32)
        folded[0, l] = n + s
        folded[1, l] = n - s
    for sign in range(2):
        pieces = [lambda l=l: folded[sign, l] for l in range(half)]
        for tile in range(5):
            for fi in range(3):
                value = gather_lanes(pieces, ROWS, ROWS * fi, tile, lane)
                first = pl.multiple_of((3 * ft + fi) * 40, 8)
                wide[5 * sign + tile, pl.ds(first, 40), :] = value


def legendre_pair(q, p, limits, wide, main, extra, synths, joined, levels):
    def operand(sign):
        parts = []
        for par in range(2):
            for c in range(2):
                row = 2 * q + c
                if par == 1:
                    row += 24 - 20 * lax.div(q, 8)
                parts.append(strided(wide, 5 * sign, 5, row, FLD, 40))
        return jnp.concatenate(parts, axis=0).astype(BF16)

    sym, anti = operand(0), operand(1)
    lane96 = lax.broadcasted_iota(jnp.int32, (96, 128), 1)
    z_sym = jnp.dot(sym, main[q, :, 0:256], preferred_element_type=F32)
    z_anti = jnp.dot(anti, main[q, :, 256:512], preferred_element_type=F32)
    tail = main[q, :, 512:640]
    z_tail = jnp.where(
        lane96 < 64,
        jnp.dot(sym, tail, preferred_element_type=F32),
        jnp.dot(anti, tail, preferred_element_type=F32),
    )
    z_extra = jnp.dot(sym, extra[...], preferred_element_type=F32)
    z_extra = jnp.sum(jnp.where(lane96 == q, z_extra, 0.0), axis=1, keepdims=True)
    first_sym = lax.shift_right_logical(641 - p, 1)
    first_anti = lax.shift_right_logical(640 - p, 1)
    parity = lax.bitwise_and(p, 1)

    def choose(z, rank, first):
        taken = jnp.where(rank < first, 1, 0) ^ parity
        return jnp.where(taken == 1, z[0:48], z[48:96])

    lane = lax.broadcasted_iota(jnp.int32, (48, 128), 1)
    rank = lax.broadcasted_iota(jnp.int32, (48, 256), 1)
    z_sym = choose(z_sym, rank, first_sym).astype(BF16)
    z_anti = choose(z_anti, rank, first_anti).astype(BF16)
    z_tail = jnp.where(
        lane < 64,
        choose(z_tail, lane + 256, first_sym),
        choose(z_tail, lane + 192, first_anti),
    )
    z_tail = z_tail.astype(BF16).astype(F32)
    z_extra = choose(jnp.broadcast_to(z_extra, (96, 128)), lane * 0 + 320, first_sym)
    sym32, anti32 = z_sym.astype(F32), z_anti.astype(F32)
    low, high = pltpu.roll(anti32[:, 0:128], 65, 1), pltpu.roll(anti32[:, 128:256], 65, 1)
    end = pltpu.roll(z_tail, 1, 1)
    own = pl.ds(pl.multiple_of(q * 48, 48), 48)
    joined[0, own] = sym32[:, 0:128]
    joined[1, own] = sym32[:, 128:256]
    joined[2, own] = jnp.where(lane < 64, z_tail, jnp.where(lane == 64, z_extra, low))
    joined[3, own] = jnp.where(lane < 65, low, high)
    joined[4, own] = jnp.where(lane < 65, high, end)
    joined[5, own] = end

    for level, place in enumerate((0, 3, 5)):
        size = LEVELS[level]
        h = size // 2
        degree = p + 2 * rank
        kept_sym = jnp.where(degree <= limits[level], sym32, 0.0).astype(BF16)[:, 0:h]
        kept_anti = jnp.where(degree + 1 <= limits[level], anti32, 0.0).astype(BF16)[:, 0:h]
        even = jnp.dot(kept_sym, synths[level][q, 0], preferred_element_type=F32)
        odd = jnp.dot(kept_anti, synths[level][q, 1], preferred_element_type=F32)
        for sign, value in enumerate((even + odd, even - odd)):
            for k in range(0, size, 128):
                width = min(128, size - k)
                levels[6 * sign + place + k // 128, own, 0:width] = value[:, k : k + width]


def make_pickers(pickers):
    row = lax.broadcasted_iota(jnp.int32, (640, 1), 0).astype(F32)
    lane_of = lax.broadcasted_iota(jnp.int32, (640, 768), 1).astype(F32)
    block = jnp.floor((row + 0.5) * (1.0 / 40))
    t = row - 40.0 * block
    for sign in range(2):
        at = [t, t - 24.0, t - 34.0]
        if sign == 1:
            at = [19.0 - t, 33.0 - t, 38.0 - t]
        target = jnp.where(
            t < 20.0,
            20.0 * block + at[0],
            jnp.where(
                (t >= 24.0) & (t < 34.0),
                384.0 + 10.0 * block + at[1],
                jnp.where((t >= 34.0) & (t < 39.0), 640.0 + 5.0 * block + at[2], -1.0),
            ),
        )
        pickers[sign] = jnp.where(lane_of == target, 1.0, 0.0).astype(BF16)


def turn_levels(part, levels, turned, pickers, blocks):
    half = NLAT // 2
    base = 0 if part == 0 else 2 * EARLY * FLD
    size = blocks.shape[2]
    for sign in range(2):
        if part == 0:
            for f in range(FLD):
                value = strided(levels, 6 * sign, 6, f, 2 * EARLY, FLD)
                turned[2 * EARLY * f : 2 * EARLY * (f + 1)] = value
        else:
            for i in range(2 * (PAIR - EARLY)):
                first = base + FLD * i
                tiles = [levels[6 * sign + k, first : first + FLD, :] for k in range(6)]
                first = base + 32 * i
                turned[first : first + FLD] = jnp.concatenate(tiles, axis=1)
        picked = lax.dot_general(
            pickers[sign],
            turned[base : base + size].astype(BF16),
            NT,
            preferred_element_type=F32,
        )
        picked = picked.reshape(half, 40, size).astype(BF16)
        if sign == 0:
            blocks[0:half] = picked
        else:
            for m in range(half):
                blocks[NLAT - 1 - m] = picked[m]


def swap_units(values, width):
    lane = lax.broadcasted_iota(jnp.int32, values[0].shape, 1)
    values = list(values)
    k = 1
    while k < len(values):
        upper = (lane & (k * width)) != 0
        for a in range(len(values)):
            if a & k == 0:
                low, high = values[a], values[a + k]
                values[a] = jnp.where(upper, pltpu.roll(high, k * width, 1), low)
                values[a + k] = jnp.where(upper, high, pltpu.roll(low, 128 - k * width, 1))
        k *= 2
    return values


def spread_early(arrived, wide):
    def group(g):
        lanes = pl.ds(pl.multiple_of(g * 128, 128), 128)
        for tile in range(4):
            values = [arrived[8 * tile + a, :, lanes].astype(F32) for a in range(8)]
            for a, value in enumerate(swap_units(values, 16)):
                wide[tile, pl.ds(8 * g + a, 40, stride=FLD), :] = value

    each(0, 3, group)


def spread_late(arrived, wide):
    def rows(b):
        own = pl.ds(pl.multiple_of(8 * b, 8), 8)
        values = [arrived[l, own, :].astype(F32) for l in range(NLAT)]
        for f, value in enumerate(swap_units(values, 1)[0:FLD]):
            wide[4, pl.ds(8 * FLD * b + f, 8, stride=FLD), :] = value

    each(0, 5, rows)


LEVEL_ROWS = ((0, 480), (576, 240), (816, 120))


def main_kernel(
    assign_s, limits, assign_v, fields_in, legendre_in, s1_in, s2_in, s3_in,
    spec_out, rows_out, p1_out, p2_out, p3_out, t1_out, t2_out, t3_out,
    raw, main, extra, columns, table, fields, folded_rows, y, x, folded, wide, joined, levels, turned,
    spec, early, late, early_in, late_in, rows_v, pickers, cols, perm, s1, s2, s3, t1, t2, t3,
    p1, p2, p3,
    raw_sem, field_sem, load_sem, store_sem, y_send, y_recv, near_send, near_recv,
    far_send, far_recv, extra_send, extra_recv, block_send, block_recv,
):
    lat = lax.axis_index("lat")
    fld = lax.axis_index("fld")
    rows = legendre_in.shape[1]
    own = pl.ds(pl.multiple_of(fld * rows, rows), rows)
    synths = (s1, s2, s3)

    def raw_copy(q):
        return pltpu.make_async_copy(legendre_in.at[q], raw.at[q], raw_sem.at[q])

    def field_copy(g):
        part = pl.ds(g * 6, 6)
        return pltpu.make_async_copy(fields_in.at[part], fields.at[part], field_sem.at[g])

    loads = [
        pltpu.make_async_copy(a, b, load_sem.at[k])
        for k, (a, b) in enumerate(((s1_in, s1), (s2_in, s2), (s3_in, s3)))
    ]
    tables = [
        pltpu.make_async_copy(a.at[pl.ds(DEEP, 128)], b, store_sem.at[k])
        for k, (a, b) in enumerate(((t1, t1_out), (t2, t2_out), (t3, t3_out)))
    ]
    each(0, PAIR, lambda q: raw_copy(q).start())
    all_greeted = greet()
    each(0, 4, lambda g: field_copy(g).start())
    for copy in loads:
        copy.start()
    extra[own] = jnp.zeros((rows, 128), BF16)

    def shard(q, k):
        s = lax.rem(fld + k, NFLD)
        return main.at[q, pl.ds(pl.multiple_of(s * rows, rows), rows)]

    def near(h, way):
        pair = main.at[pl.ds(2 * h, 2), own]
        return to_fld(pair, near_send, near_recv.at[way, h], 1 + 2 * way)

    def near_last(q, way):
        return to_fld(shard(q, 0), near_send, near_recv.at[way, q - 4], 1 + 2 * way)

    def far(q, way):
        return to_fld(shard(q, 3 - 2 * way), far_send, far_recv.at[q], 1 + 2 * way)

    def extra_copy(k):
        return to_fld(columns.at[fld], extra_send.at[k - 1], extra_recv.at[k - 1], k)

    def start_near(h):
        near(h, 0).start()
        near(h, 1).start()

    def start_last():
        near_last(8, 0).start()
        near_last(9, 1).start()
        near_last(9, 0).start()
        near_last(8, 1).start()

    def pack_one(q):
        raw_copy(q).wait()
        pack_pair(q, raw, main, extra, own)

    pack_one(0)
    pack_one(1)
    all_greeted()
    start_near(0)
    pack_one(2)
    pack_one(3)
    folded_rows[...] = jnp.zeros_like(folded_rows)
    make_columns(assign_v, cols, 0)
    make_columns(assign_v, cols, 1)
    make_turner(perm)

    def fill(b):
        first = pl.multiple_of(b * 64, 64)

        def store(a, value):
            table[pl.ds(first, 64), 128 * a : 128 * a + 128] = value.astype(BF16)

        fill_table(cols, first, 64, LON, 1.0 / math.sqrt(LON), 10, store)

    each(0, 24, fill)
    start_near(1)

    def lanes_of(g):
        return pl.ds(pl.multiple_of(g * 256, 256), 256)

    def y_copy(g, k):
        return to_lat(
            y.at[lat_peer(k), :, lanes_of(g)],
            x.at[lat, :, lanes_of(g)],
            y_send.at[g],
            y_recv.at[g],
            k,
        )

    def y_wait(g):
        part = pl.ds(0, NLAT - 1)
        both = to_lat(
            y.at[part, :, lanes_of(g)], x.at[part, :, lanes_of(g)], y_send.at[g], y_recv.at[g], 1
        )
        both.wait_send()
        both.wait_recv()

    def relay(h):
        near(h, 0).wait_recv()
        far(2 * h, 0).start()
        near(h, 1).wait_recv()
        far(2 * h + 1, 1).start()

    def transform(g):
        field_copy(g).wait()
        dft_group(g, table, folded_rows, perm, fields, y, lanes_of(g))
        x[lat, :, lanes_of(g)] = y[lat, :, lanes_of(g)]

    def send_group(g):
        each(1, NLAT, lambda k: y_copy(g, k).start())

    def group(g):
        transform(g)
        pack_one(2 * g + 4)
        pack_one(2 * g + 5)
        send_group(g)

        @pl.when(g < 2)
        def _():
            start_near(g + 2)

        @pl.when(g > 0)
        def _():
            relay(g - 1)

    each(0, 3, group)
    transform(3)
    send_group(3)
    unit = lax.broadcasted_iota(jnp.int32, (16, 128), 0)
    unit = jnp.where(unit == lax.broadcasted_iota(jnp.int32, (16, 128), 1), 1.0, 0.0).astype(BF16)
    columns[fld] = jnp.zeros((16, 256), BF16)
    columns[fld, :, 0:rows] = lax.dot_general(
        unit, extra[own], NT, preferred_element_type=F32
    ).astype(BF16)

    levels[...] = jnp.zeros_like(levels)
    turned[...] = jnp.zeros_like(turned)
    make_pickers(pickers)
    for k in range(1, NFLD):
        extra_copy(k).start()
    make_columns(assign_v, cols, 2)

    def fill_inverse(b):
        first = pl.multiple_of(b * 64, 64)
        for out, size, tiles in ((t1, 1280, 10), (t2, 640, 5), (t3, 320, 3)):

            def store(a, value, out=out):
                out[pl.ds(first, 64), 128 * a : 128 * a + 128] = value.astype(BF16)

            fill_table(cols, 1536 + first, 64, size, 1.0 / math.sqrt(size), tiles, store)

    each(0, 12, fill_inverse)
    for copy in tables:
        copy.start()

    def take_group(g):
        y_wait(g)
        fold_fields(2 * g, x, folded, wide)
        fold_fields(2 * g + 1, x, folded, wide)

        @pl.when(g == 0)
        def _():
            relay(2)

        @pl.when(g == 2)
        def _():
            relay(3)
            start_last()

    each(0, 4, take_group)
    for copy in loads:
        copy.wait()
    for k in range(1, NFLD):
        extra_copy(k).wait()
    for k in range(NFLD):
        back = lax.dot_general(
            columns[k, :, 0:rows], unit, (((0,), (0,)), ((), ())), preferred_element_type=F32
        )
        extra[rows * k : rows * k + rows] = back.astype(BF16)

    parts = ((early, early_in), (late, late_in))

    def block_copy(part, k):
        return to_lat(
            parts[part][0].at[lat_peer(k)],
            parts[part][1].at[lat],
            block_send.at[part],
            block_recv.at[part],
            k,
        )

    def pair(q):
        way = lax.rem(q, 2)
        far(q, way).wait_recv()
        p = assign_s[PAIR * lat + q]
        legendre_pair(q, p, limits, wide, main, extra, synths, joined, levels)

    def send_part(part):
        turn_levels(part, levels, turned, pickers, parts[part][0])
        parts[part][1][lat] = parts[part][0][lat]
        each(1, NLAT, lambda k: block_copy(part, k).start())

    def take_part(part):
        count = pl.ds(0, NLAT - 1)
        both = to_lat(
            parts[part][0].at[count], parts[part][1].at[count], block_send.at[part],
            block_recv.at[part], 1,
        )
        both.wait_send()
        both.wait_recv()

    each(0, EARLY, pair)
    send_part(0)
    near_last(8, 0).wait_recv()
    far(8, 0).start()
    near_last(9, 1).wait_recv()
    far(9, 1).start()
    near_last(8, 1).wait_recv()
    near_last(9, 0).wait_recv()
    each(EARLY, PAIR, pair)
    send_part(1)

    def field(f):
        part = strided(joined, 0, 6, f, 2 * PAIR, FLD)
        spec[f] = part[:, 0:641].reshape(PAIR, 2, 641).astype(BF16)

    each(0, FLD, field)
    spec_copy = pltpu.make_async_copy(spec, spec_out, store_sem.at[4])
    spec_copy.start()

    first_two = main.at[:, pl.ds(0, 2 * rows)]
    to_fld(first_two, near_send, near_recv.at[0, 0], 1).wait_send()
    to_fld(main.at[:, pl.ds(0, rows)], far_send, far_recv.at[0], 1).wait_send()
    take_part(0)
    spread_early(early_in, wide)
    for k, (table_k, p) in enumerate(((t1, p1), (t2, p2), (t3, p3))):
        first, count = LEVEL_ROWS[k]
        tiles = [wide[tile, first : first + count, :] for tile in range(4)]
        lhs = jnp.concatenate(tiles, axis=1).astype(BF16)
        p[...] = jnp.dot(lhs, table_k[0:DEEP], preferred_element_type=F32)
    products = [
        pltpu.make_async_copy(a, b, store_sem.at[5 + k])
        for k, (a, b) in enumerate(((p1, p1_out), (p2, p2_out), (p3, p3_out)))
    ]
    for copy in products:
        copy.start()
    take_part(1)
    spread_late(late_in, wide)
    done = 0
    for first, count in LEVEL_ROWS:
        rows_v[done : done + count] = wide[4, first : first + count, :].astype(BF16)
        done += count
    rows_copy = pltpu.make_async_copy(rows_v, rows_out, store_sem.at[3])
    rows_copy.start()
    for copy in products:
        copy.wait()
    for copy in tables:
        copy.wait()
    spec_copy.wait()
    rows_copy.wait()


def main_step(assign, limits, fields, legendre_t, synths):
    hbm = pl.BlockSpec(memory_space=pltpu.HBM)
    vmem = pl.BlockSpec(memory_space=pltpu.VMEM)
    smem = pl.BlockSpec(memory_space=pltpu.SMEM)
    dma = pltpu.SemaphoreType.DMA
    rows = legendre_t.shape[1]
    synths = [s.reshape(PAIR, 2, m // 2, m) for s, m in zip(synths, LEVELS)]
    wides = (1280, 640, 384)
    return pl.pallas_call(
        main_kernel,
        in_specs=[smem, smem, vmem] + [hbm] * 5,
        out_specs=[hbm] * 8,
        out_shape=[
            jax.ShapeDtypeStruct((FLD, PAIR, 2, 641), BF16),
            jax.ShapeDtypeStruct((FLD * sum(SENT), 128), BF16),
            *[jax.ShapeDtypeStruct((n, w), F32) for (_, n), w in zip(LEVEL_ROWS, wides)],
            *[jax.ShapeDtypeStruct((128, w), BF16) for w in wides],
        ],
        scratch_shapes=[
            pltpu.VMEM((PAIR, rows, 641), BF16),
            pltpu.VMEM((PAIR, NFLD * rows, 640), BF16),
            pltpu.VMEM((NFLD * rows, 128), BF16),
            pltpu.VMEM((NFLD, 16, 256), BF16),
            pltpu.VMEM((1536, LON // 2), BF16),
            pltpu.VMEM((FLD, ROWS, LON), BF16),
            pltpu.VMEM((256, LON // 2), BF16),
            pltpu.VMEM((NLAT, 40, 1024), BF16),
            pltpu.VMEM((NLAT, 40, 1024), BF16),
            pltpu.VMEM((2, NLAT // 2, 40, 128), F32),
            pltpu.VMEM((10, 40 * FLD, 128), F32),
            pltpu.VMEM((6, 48 * PAIR, 128), F32),
            pltpu.VMEM((12, 48 * PAIR, 128), F32),
            pltpu.VMEM((512, 768), F32),
            pltpu.VMEM((FLD, PAIR, 2, 641), BF16),
            pltpu.VMEM((NLAT, 40, 384), BF16),
            pltpu.VMEM((NLAT, 40, 128), BF16),
            pltpu.VMEM((NLAT, 40, 384), BF16),
            pltpu.VMEM((NLAT, 40, 128), BF16),
            pltpu.VMEM((FLD * sum(SENT), 128), BF16),
            pltpu.VMEM((2, 640, 768), BF16),
            pltpu.VMEM((2304, 8), F32),
            pltpu.VMEM((256, 256), BF16),
            *[pltpu.VMEM(s.shape, BF16) for s in synths],
            *[pltpu.VMEM((768, w), BF16) for w in wides],
            *[pltpu.VMEM((n, w), F32) for (_, n), w in zip(LEVEL_ROWS, wides)],
            dma((PAIR,)), dma((4,)), dma((3,)), dma((8,)),
            dma((4,)), dma((4,)), dma, dma((2, 6)), dma, dma((PAIR,)),
            dma((NFLD - 1,)), dma((NFLD - 1,)), dma((2,)), dma((2,)),
        ],
        compiler_params=pltpu.CompilerParams(
            collective_id=0, has_side_effects=True, vmem_limit_bytes=64 * 1000 * 1000
        ),
    )(assign, limits, assign, fields, legendre_t, *synths)


CHUNKS = ((0, 0, 6), (0, 6, 6), (0, 12, 8), (1, 0, 10), (2, 0, 5))


def inverse_kernel(
    rows_in, spec_in, p1_in, p2_in, p3_in, t1_in, t2_in, t3_in,
    spec_out, o1_out, o2_out, o3_out,
    rows, spec, p1, p2, p3, t1, t2, t3, o1, o2, o3, in_sem, part_sem, out_sem,
):
    sums, outs = (p1, p2, p3), (o1, o2, o3)
    sources, results, tables = (p1_in, p2_in, p3_in), (o1_out, o2_out, o3_out), (t1, t2, t3)
    small = [
        pltpu.make_async_copy(a, b, in_sem.at[k])
        for k, (a, b) in enumerate(
            ((rows_in, rows), (t1_in, t1), (t2_in, t2), (t3_in, t3), (spec_in, spec))
        )
    ]
    loads, stores = [], []
    for k, (level, first, count) in enumerate(CHUNKS):
        part = pl.ds(FLD * first, FLD * count)
        loads.append(
            pltpu.make_async_copy(
                sources[level].at[part], sums[level].at[part], part_sem.at[k]
            )
        )
        part = pl.ds(first, count)
        stores.append(
            pltpu.make_async_copy(outs[level].at[part], results[level].at[part], out_sem.at[k])
        )
    for copy in small[0:2] + loads[0:3] + small[2:4] + loads[3:5] + small[4:5]:
        copy.start()
    small[0].wait()
    spec_store = pltpu.make_async_copy(spec, spec_out, out_sem.at[len(CHUNKS)])
    begin = (0, 20, 30)
    for k, (level, first, count) in enumerate(CHUNKS):
        if first == 0:
            small[1 + level].wait()
        loads[k].wait()
        start = FLD * (begin[level] + first)
        lhs = rows[start : start + FLD * count]
        z = jnp.dot(lhs, tables[level][...], preferred_element_type=F32)
        z = z + sums[level][FLD * first : FLD * (first + count)]
        size = outs[level].shape[2]
        outs[level][first : first + count] = z[:, 0:size].reshape(count, FLD, size)
        stores[k].start()
    small[4].wait()
    spec_store.start()
    for copy in stores:
        copy.wait()
    spec_store.wait()


def inverse_step(rows, spectrum, products, tables):
    shapes = [(n, FLD, 4 * m) for n, m in zip(SENT, LEVELS)]
    hbm = pl.BlockSpec(memory_space=pltpu.HBM)
    dma = pltpu.SemaphoreType.DMA
    inputs = (rows, spectrum, *products, *tables)
    return pl.pallas_call(
        inverse_kernel,
        in_specs=[hbm] * 8,
        out_specs=[hbm] * 4,
        out_shape=[jax.ShapeDtypeStruct(spectrum.shape, spectrum.dtype)]
        + [jax.ShapeDtypeStruct(s, F32) for s in shapes],
        scratch_shapes=[pltpu.VMEM(a.shape, a.dtype) for a in inputs]
        + [pltpu.VMEM(s, F32) for s in shapes]
        + [dma((5,)), dma((len(CHUNKS),)), dma((len(CHUNKS) + 1,))],
    )(*inputs)


def on_device(grid_fields, assign, limits, legendre, synth_one, synth_two, synth_three):
    spectrum, rows, *rest = main_step(
        assign,
        limits,
        grid_fields,
        jnp.transpose(legendre, (0, 2, 1)),
        (synth_one, synth_two, synth_three),
    )
    spectrum, *grids = inverse_step(rows, spectrum, rest[0:3], rest[3:6])
    return (
        jnp.transpose(spectrum, (0, 2, 1, 3)),
        *[jnp.transpose(g, (1, 0, 2)) for g in grids],
    )


def solution(mesh):
    return jax.shard_map(
        on_device,
        mesh=mesh,
        in_specs=(
            P("fld", "lat", None),
            P(),
            P(),
            P("lat", None, "fld"),
            P("lat", None, None),
            P("lat", None, None),
            P("lat", None, None),
        ),
        out_specs=(
            P("fld", None, "lat", None),
            P("fld", "lat", None),
            P("fld", "lat", None),
            P("fld", "lat", None),
        ),
        check_vma=False,
    )
```

```python
import math

import jax
import jax.numpy as jnp
from jax import lax
from jax.experimental import pallas as pl
from jax.experimental.pallas import tpu as pltpu
from jax.sharding import PartitionSpec as P

MESH = pl.DeviceIdType.MESH
F32 = jnp.float32
BF16 = jnp.bfloat16
NLAT = 32
NFLD = 4
FLD = 24
ROWS = 40
LON = 2560
PAIR = 10
SENT = (20, 10, 5)
LEVELS = (320, 160, 80)
NT = (((1,), (1,)), ((), ()))
EARLY = 8
DEEP = 2 * EARLY * NLAT


def sincos(turns):
    quarter = jnp.floor(turns * 4.0 + 0.5)
    y = (turns * 4.0 - quarter) * (math.pi / 2)
    y2 = y * y
    s = y * (1.0 + y2 * (-1.0 / 6 + y2 * (1.0 / 120 - y2 * (1.0 / 5040))))
    c = 1.0 + y2 * (-0.5 + y2 * (1.0 / 24 + y2 * (-1.0 / 720 + y2 * (1.0 / 40320))))
    k = quarter - 4.0 * jnp.floor(quarter * 0.25)
    odd = (k == 1.0) | (k == 3.0)
    sin_v = jnp.where(odd, c, s)
    cos_v = jnp.where(odd, s, c)
    sin_v = jnp.where(k >= 2.0, -sin_v, sin_v)
    cos_v = jnp.where((k == 1.0) | (k == 2.0), -cos_v, cos_v)
    return cos_v, sin_v


def turns_of(product, period):
    return (product - period * jnp.floor(product * (1.0 / period))) * (1.0 / period)


def fill_table(cols_ref, first, count, period, scale, tiles, store):
    wave = jnp.broadcast_to(cols_ref[pl.ds(first, count), 0:1], (count, 128))
    amp = jnp.broadcast_to(cols_ref[pl.ds(first, count), 1:2], (count, 128)) * scale
    comp = jnp.broadcast_to(cols_ref[pl.ds(first, count), 2:3], (count, 128))
    lane = lax.broadcasted_iota(jnp.int32, (count, 128), 1).astype(F32)
    cos_v, sin_v = sincos(turns_of(wave * lane + comp * (period // 4), float(period)))
    cos_d, sin_d = sincos(turns_of(wave * 128.0, float(period)))
    cos_v, sin_v = cos_v * amp, sin_v * amp
    for a in range(tiles):
        store(a, cos_v)
        if a + 1 < tiles:
            cos_v, sin_v = cos_v * cos_d - sin_v * sin_d, sin_v * cos_d + cos_v * sin_d


def lat_peer(k):
    return lax.rem(lax.axis_index("lat") + k, NLAT)


def greet():
    barrier = pltpu.get_barrier_semaphore()
    fld = lax.axis_index("fld")
    lat = lax.axis_index("lat")

    def one(k, carry):
        pl.semaphore_signal(barrier, inc=1, device_id=(lat_peer(k), fld), device_id_type=MESH)
        return carry

    lax.fori_loop(1, NLAT, one, 0)
    for k in range(1, NFLD):
        pl.semaphore_signal(
            barrier, inc=1, device_id=(lat, lax.rem(fld + k, NFLD)), device_id_type=MESH
        )
    return lambda: pl.semaphore_wait(barrier, NLAT + NFLD - 2)


def to_lat(src, dst, send_sem, recv_sem, k):
    return pltpu.make_async_remote_copy(
        src_ref=src,
        dst_ref=dst,
        send_sem=send_sem,
        recv_sem=recv_sem,
        device_id=(lat_peer(k), lax.axis_index("fld")),
        device_id_type=MESH,
    )


def to_fld(part, send_sem, recv_sem, k):
    fld = lax.rem(lax.axis_index("fld") + k, NFLD)
    return pltpu.make_async_remote_copy(
        src_ref=part,
        dst_ref=part,
        send_sem=send_sem,
        recv_sem=recv_sem,
        device_id=(lax.axis_index("lat"), fld),
        device_id_type=MESH,
    )


def each(first, count, act):
    def one(k, carry):
        act(k)
        return carry

    lax.fori_loop(first, count, one, 0)


def pack_pair(q, raw, main, extra, own):
    a = raw[q].astype(F32)
    t = [a[:, 128 * k : 128 * k + 128] for k in range(5)]
    last = a[:, 640:641]
    lane = lax.broadcasted_iota(jnp.int32, (a.shape[0], 128), 1)
    r = [None, None] + [pltpu.roll(t[k], 63, 1) for k in (2, 3, 4)]
    main[q, own, 0:128] = t[0].astype(BF16)
    main[q, own, 128:256] = t[1].astype(BF16)
    main[q, own, 256:384] = jnp.where(lane < 63, r[2], r[3]).astype(BF16)
    main[q, own, 384:512] = jnp.where(lane < 63, r[3], r[4]).astype(BF16)
    tail = jnp.where(lane < 127, pltpu.roll(t[4], 127, 1), last)
    main[q, own, 512:640] = jnp.where(lane < 64, t[2], tail).astype(BF16)
    column = jnp.sum(jnp.where(lane == 64, t[2], 0.0), axis=1, keepdims=True)
    extra[own] = jnp.where(lane == q, column, extra[own].astype(F32)).astype(BF16)


def dft_group(g, table, folded, perm_ref, fields, y_ref, lanes):
    x = fields[pl.ds(g * 6, 6)].astype(F32)
    low = x[:, :, : LON // 2].reshape(240, LON // 2)
    high = x[:, :, LON // 2 :].reshape(240, LON // 2)
    parts = []
    for par in range(2):
        x = low + high if par == 0 else low - high
        folded[0:120] = x[0:120].astype(BF16)
        folded[128:248] = x[120:240].astype(BF16)
        y = lax.dot_general(
            table[768 * par : 768 * par + 768], folded[...], NT, preferred_element_type=F32
        )
        y = jnp.dot(y.astype(BF16), perm_ref[...], preferred_element_type=F32)
        parts.append((y[0:512].reshape(NLAT, 16, 256), y[512:768].reshape(NLAT, 8, 256)))
    (first, mid), (last, other) = parts
    y_ref[:, :, lanes] = jnp.concatenate([first, mid + other, last], axis=1).astype(BF16)


def make_columns(assign_ref, cols, part):
    p = assign_ref[...].reshape(1, -1).astype(F32)
    total = 2.0 * assign_ref.shape[0] - 1.0
    even = jnp.where(p - 2.0 * jnp.floor(p * 0.5) > 0.5, total - p, p)
    value = (even, total - even, p)[part]
    high = jnp.floor(value * (1.0 / 16))
    place = lax.broadcasted_iota(jnp.int32, (8, value.shape[1]), 0)
    digits = jnp.where(place == 0, high, jnp.where(place == 1, value - 16.0 * high, 0.0))
    r = lax.broadcasted_iota(jnp.int32, (768, 1), 0).astype(F32)
    if part < 2:
        rest = r >= 512.0
        s = jnp.where(rest, r - 512.0, r)
        l = jnp.where(rest, jnp.floor((s + 0.5) * (1.0 / 8)), jnp.floor((s + 0.5) * (1.0 / 16)))
        i = s - jnp.where(rest, 8.0, 16.0) * l
        if part == 0:
            valid = jnp.logical_not(rest) | (i < 4.0)
            q = jnp.floor(i * 0.5) + jnp.where(rest, 8.0, 0.0)
        else:
            valid = jnp.logical_not(rest) | (i >= 4.0)
            q = jnp.floor(i * 0.5) + jnp.where(rest, 6.0, 0.0)
    else:
        late = r >= 512.0
        s = jnp.where(late, r - 512.0, r)
        valid = r < 640.0
        high_part = jnp.floor((s + 0.5) * jnp.where(late, 1.0 / 32, 1.0 / 16))
        low_part = s - jnp.where(late, 32.0, 16.0) * high_part
        l = jnp.where(late, low_part, high_part)
        i = jnp.where(late, high_part, low_part)
        q = jnp.floor(i * 0.5) + jnp.where(late, 8.0, 0.0)
    slot = jnp.where(valid, 10.0 * l + q, -1.0)
    lane = lax.broadcasted_iota(jnp.int32, (768, value.shape[1]), 1).astype(F32)
    picker = jnp.where(lane == slot, 1.0, 0.0).astype(BF16)
    found = lax.dot_general(picker, digits.astype(BF16), NT, preferred_element_type=F32)
    wave = 16.0 * found[:, 0:1] + found[:, 1:2]
    amp = jnp.where(valid, 1.0, 0.0)
    if part == 2:
        amp = amp * jnp.where(wave > 0.5, 2.0, 1.0)
    rows = slice(768 * part, 768 * part + 768)
    cols[rows, 0:1] = wave
    cols[rows, 1:2] = amp
    cols[rows, 2:3] = i - 2.0 * jnp.floor(i * 0.5)


def make_turner(perm):
    u = lax.broadcasted_iota(jnp.int32, (256, 256), 0).astype(F32)
    v = lax.broadcasted_iota(jnp.int32, (256, 256), 1).astype(F32)
    inner = v - 128.0 * jnp.floor(v * (1.0 / 128))
    t = inner - 40.0 * jnp.floor((inner + 0.5) * (1.0 / 40))
    source = jnp.where(lax.axis_index("lat") >= NLAT // 2, v + 39.0 - 2.0 * t, v)
    perm[...] = jnp.where((u == source) & (inner < 120.0), 1.0, 0.0).astype(BF16)


def gather_lanes(pieces, width, offset, tile, lane):
    first, last = 128 * tile // width, min((128 * tile + 127) // width, len(pieces) - 1)
    total = None
    for l in range(first, last + 1):
        turned = pltpu.roll(pieces[l](), (width * l - offset) % 128, 1)
        start = width * l - 128 * tile
        total = turned if total is None else jnp.where(lane >= start, turned, total)
    return total


def strided(ref, lead, tiles, first, count, step):
    parts = [ref[lead + k, pl.ds(first, count, stride=step), :] for k in range(tiles)]
    return jnp.concatenate(parts, axis=1)


def fold_fields(ft, x_ref, folded, wide):
    half = NLAT // 2
    lane = lax.broadcasted_iota(jnp.int32, (40, 128), 1)
    lanes = pl.ds(pl.multiple_of(ft * 128, 128), 128)
    for l in range(half):
        n = x_ref[l, :, lanes].astype(F32)
        s = x_ref[NLAT - 1 - l, :, lanes].astype(F32)
        folded[0, l] = n + s
        folded[1, l] = n - s
    for sign in range(2):
        pieces = [lambda l=l: folded[sign, l] for l in range(half)]
        for tile in range(5):
            for fi in range(3):
                value = gather_lanes(pieces, ROWS, ROWS * fi, tile, lane)
                first = pl.multiple_of((3 * ft + fi) * 40, 8)
                wide[5 * sign + tile, pl.ds(first, 40), :] = value


def legendre_pair(q, p, limits, wide, main, extra, synths, joined, levels):
    def operand(sign):
        parts = []
        for par in range(2):
            for c in range(2):
                row = 2 * q + c
                if par == 1:
                    row += 24 - 20 * lax.div(q, 8)
                parts.append(strided(wide, 5 * sign, 5, row, FLD, 40))
        return jnp.concatenate(parts, axis=0).astype(BF16)

    sym, anti = operand(0), operand(1)
    lane96 = lax.broadcasted_iota(jnp.int32, (96, 128), 1)
    z_sym = jnp.dot(sym, main[q, :, 0:256], preferred_element_type=F32)
    z_anti = jnp.dot(anti, main[q, :, 256:512], preferred_element_type=F32)
    tail = main[q, :, 512:640]
    z_tail = jnp.where(
        lane96 < 64,
        jnp.dot(sym, tail, preferred_element_type=F32),
        jnp.dot(anti, tail, preferred_element_type=F32),
    )
    z_extra = jnp.dot(sym, extra[...], preferred_element_type=F32)
    z_extra = jnp.sum(jnp.where(lane96 == q, z_extra, 0.0), axis=1, keepdims=True)
    first_sym = lax.shift_right_logical(641 - p, 1)
    first_anti = lax.shift_right_logical(640 - p, 1)
    parity = lax.bitwise_and(p, 1)

    def choose(z, rank, first):
        taken = jnp.where(rank < first, 1, 0) ^ parity
        return jnp.where(taken == 1, z[0:48], z[48:96])

    lane = lax.broadcasted_iota(jnp.int32, (48, 128), 1)
    rank = lax.broadcasted_iota(jnp.int32, (48, 256), 1)
    z_sym = choose(z_sym, rank, first_sym).astype(BF16)
    z_anti = choose(z_anti, rank, first_anti).astype(BF16)
    z_tail = jnp.where(
        lane < 64,
        choose(z_tail, lane + 256, first_sym),
        choose(z_tail, lane + 192, first_anti),
    )
    z_tail = z_tail.astype(BF16).astype(F32)
    z_extra = choose(jnp.broadcast_to(z_extra, (96, 128)), lane * 0 + 320, first_sym)
    sym32, anti32 = z_sym.astype(F32), z_anti.astype(F32)
    low, high = pltpu.roll(anti32[:, 0:128], 65, 1), pltpu.roll(anti32[:, 128:256], 65, 1)
    end = pltpu.roll(z_tail, 1, 1)
    own = pl.ds(pl.multiple_of(q * 48, 48), 48)
    joined[0, own] = sym32[:, 0:128]
    joined[1, own] = sym32[:, 128:256]
    joined[2, own] = jnp.where(lane < 64, z_tail, jnp.where(lane == 64, z_extra, low))
    joined[3, own] = jnp.where(lane < 65, low, high)
    joined[4, own] = jnp.where(lane < 65, high, end)
    joined[5, own] = end

    for level, place in enumerate((0, 3, 5)):
        size = LEVELS[level]
        h = size // 2
        degree = p + 2 * rank
        kept_sym = jnp.where(degree <= limits[level], sym32, 0.0).astype(BF16)[:, 0:h]
        kept_anti = jnp.where(degree + 1 <= limits[level], anti32, 0.0).astype(BF16)[:, 0:h]
        even = jnp.dot(kept_sym, synths[level][q, 0], preferred_element_type=F32)
        odd = jnp.dot(kept_anti, synths[level][q, 1], preferred_element_type=F32)
        for sign, value in enumerate((even + odd, even - odd)):
            for k in range(0, size, 128):
                width = min(128, size - k)
                levels[6 * sign + place + k // 128, own, 0:width] = value[:, k : k + width]


def make_pickers(pickers):
    row = lax.broadcasted_iota(jnp.int32, (640, 1), 0).astype(F32)
    lane_of = lax.broadcasted_iota(jnp.int32, (640, 768), 1).astype(F32)
    block = jnp.floor((row + 0.5) * (1.0 / 40))
    t = row - 40.0 * block
    for sign in range(2):
        at = [t, t - 24.0, t - 34.0]
        if sign == 1:
            at = [19.0 - t, 33.0 - t, 38.0 - t]
        target = jnp.where(
            t < 20.0,
            20.0 * block + at[0],
            jnp.where(
                (t >= 24.0) & (t < 34.0),
                384.0 + 10.0 * block + at[1],
                jnp.where((t >= 34.0) & (t < 39.0), 640.0 + 5.0 * block + at[2], -1.0),
            ),
        )
        pickers[sign] = jnp.where(lane_of == target, 1.0, 0.0).astype(BF16)


def turn_levels(part, levels, turned, pickers, blocks):
    half = NLAT // 2
    base = 0 if part == 0 else 2 * EARLY * FLD
    size = blocks.shape[2]
    for sign in range(2):
        if part == 0:
            for f in range(FLD):
                value = strided(levels, 6 * sign, 6, f, 2 * EARLY, FLD)
                turned[2 * EARLY * f : 2 * EARLY * (f + 1)] = value
        else:
            for i in range(2 * (PAIR - EARLY)):
                first = base + FLD * i
                tiles = [levels[6 * sign + k, first : first + FLD, :] for k in range(6)]
                first = base + 32 * i
                turned[first : first + FLD] = jnp.concatenate(tiles, axis=1)
        picked = lax.dot_general(
            pickers[sign],
            turned[base : base + size].astype(BF16),
            NT,
            preferred_element_type=F32,
        )
        picked = picked.reshape(half, 40, size).astype(BF16)
        if sign == 0:
            blocks[0:half] = picked
        else:
            for m in range(half):
                blocks[NLAT - 1 - m] = picked[m]


def swap_units(values, width):
    lane = lax.broadcasted_iota(jnp.int32, values[0].shape, 1)
    values = list(values)
    k = 1
    while k < len(values):
        upper = (lane & (k * width)) != 0
        for a in range(len(values)):
            if a & k == 0:
                low, high = values[a], values[a + k]
                values[a] = jnp.where(upper, pltpu.roll(high, k * width, 1), low)
                values[a + k] = jnp.where(upper, high, pltpu.roll(low, 128 - k * width, 1))
        k *= 2
    return values


def spread_early(arrived, wide):
    def group(g):
        lanes = pl.ds(pl.multiple_of(g * 128, 128), 128)
        for tile in range(4):
            values = [arrived[8 * tile + a, :, lanes].astype(F32) for a in range(8)]
            for a, value in enumerate(swap_units(values, 16)):
                wide[tile, pl.ds(8 * g + a, 40, stride=FLD), :] = value

    each(0, 3, group)


def spread_late(arrived, wide):
    def rows(b):
        own = pl.ds(pl.multiple_of(8 * b, 8), 8)
        values = [arrived[l, own, :].astype(F32) for l in range(NLAT)]
        for f, value in enumerate(swap_units(values, 1)[0:FLD]):
            wide[4, pl.ds(8 * FLD * b + f, 8, stride=FLD), :] = value

    each(0, 5, rows)


LEVEL_ROWS = ((0, 480), (576, 240), (816, 120))


def main_kernel(
    assign_s, limits, assign_v, fields_in, legendre_in, s1_in, s2_in, s3_in,
    spec_out, rows_out, p1_out, p2_out, p3_out, t1_out, t2_out, t3_out,
    raw, main, extra, columns, table, fields, folded_rows, y, x, folded, wide, joined, levels, turned,
    spec, early, late, early_in, late_in, rows_v, pickers, cols, perm, s1, s2, s3, t1, t2, t3,
    p1, p2, p3,
    raw_sem, field_sem, load_sem, store_sem, y_send, y_recv, near_send, near_recv,
    far_send, far_recv, extra_send, extra_recv, block_send, block_recv,
):
    lat = lax.axis_index("lat")
    fld = lax.axis_index("fld")
    rows = legendre_in.shape[1]
    own = pl.ds(pl.multiple_of(fld * rows, rows), rows)
    synths = (s1, s2, s3)

    def raw_copy(q):
        return pltpu.make_async_copy(legendre_in.at[q], raw.at[q], raw_sem.at[q])

    def field_copy(g):
        part = pl.ds(g * 6, 6)
        return pltpu.make_async_copy(fields_in.at[part], fields.at[part], field_sem.at[g])

    loads = [
        pltpu.make_async_copy(a, b, load_sem.at[k])
        for k, (a, b) in enumerate(((s1_in, s1), (s2_in, s2), (s3_in, s3)))
    ]
    tables = [
        pltpu.make_async_copy(a.at[pl.ds(DEEP, 128)], b, store_sem.at[k])
        for k, (a, b) in enumerate(((t1, t1_out), (t2, t2_out), (t3, t3_out)))
    ]
    each(0, PAIR, lambda q: raw_copy(q).start())
    all_greeted = greet()
    each(0, 4, lambda g: field_copy(g).start())
    for copy in loads:
        copy.start()
    extra[own] = jnp.zeros((rows, 128), BF16)

    def shard(q, k):
        s = lax.rem(fld + k, NFLD)
        return main.at[q, pl.ds(pl.multiple_of(s * rows, rows), rows)]

    def near(h, way):
        pair = main.at[pl.ds(2 * h, 2), own]
        return to_fld(pair, near_send, near_recv.at[way, h], 1 + 2 * way)

    def near_last(q, way):
        return to_fld(shard(q, 0), near_send, near_recv.at[way, q - 4], 1 + 2 * way)

    def far(q, way):
        return to_fld(shard(q, 3 - 2 * way), far_send, far_recv.at[q], 1 + 2 * way)

    def extra_copy(k):
        return to_fld(columns.at[fld], extra_send.at[k - 1], extra_recv.at[k - 1], k)

    def start_near(h):
        near(h, 0).start()
        near(h, 1).start()

    def start_last():
        near_last(8, 0).start()
        near_last(9, 1).start()
        near_last(9, 0).start()
        near_last(8, 1).start()

    def pack_one(q):
        raw_copy(q).wait()
        pack_pair(q, raw, main, extra, own)

    pack_one(0)
    pack_one(1)
    all_greeted()
    start_near(0)
    pack_one(2)
    pack_one(3)
    folded_rows[...] = jnp.zeros_like(folded_rows)
    make_columns(assign_v, cols, 0)
    make_columns(assign_v, cols, 1)
    make_turner(perm)

    def fill(b):
        first = pl.multiple_of(b * 64, 64)

        def store(a, value):
            table[pl.ds(first, 64), 128 * a : 128 * a + 128] = value.astype(BF16)

        fill_table(cols, first, 64, LON, 1.0 / math.sqrt(LON), 10, store)

    each(0, 24, fill)
    start_near(1)

    def lanes_of(g):
        return pl.ds(pl.multiple_of(g * 256, 256), 256)

    def y_copy(g, k):
        return to_lat(
            y.at[lat_peer(k), :, lanes_of(g)],
            x.at[lat, :, lanes_of(g)],
            y_send.at[g],
            y_recv.at[g],
            k,
        )

    def y_wait(g):
        part = pl.ds(0, NLAT - 1)
        both = to_lat(
            y.at[part, :, lanes_of(g)], x.at[part, :, lanes_of(g)], y_send.at[g], y_recv.at[g], 1
        )
        both.wait_send()
        both.wait_recv()

    def relay(h):
        near(h, 0).wait_recv()
        far(2 * h, 0).start()
        near(h, 1).wait_recv()
        far(2 * h + 1, 1).start()

    def transform(g):
        field_copy(g).wait()
        dft_group(g, table, folded_rows, perm, fields, y, lanes_of(g))
        x[lat, :, lanes_of(g)] = y[lat, :, lanes_of(g)]

    def send_group(g):
        each(1, NLAT, lambda k: y_copy(g, k).start())

    def group(g):
        transform(g)
        pack_one(2 * g + 4)
        pack_one(2 * g + 5)
        send_group(g)

        @pl.when(g < 2)
        def _():
            start_near(g + 2)

        @pl.when(g > 0)
        def _():
            relay(g - 1)

    each(0, 3, group)
    transform(3)
    send_group(3)
    unit = lax.broadcasted_iota(jnp.int32, (16, 128), 0)
    unit = jnp.where(unit == lax.broadcasted_iota(jnp.int32, (16, 128), 1), 1.0, 0.0).astype(BF16)
    columns[fld] = jnp.zeros((16, 256), BF16)
    columns[fld, :, 0:rows] = lax.dot_general(
        unit, extra[own], NT, preferred_element_type=F32
    ).astype(BF16)

    levels[...] = jnp.zeros_like(levels)
    turned[...] = jnp.zeros_like(turned)
    make_pickers(pickers)
    for k in range(1, NFLD):
        extra_copy(k).start()
    make_columns(assign_v, cols, 2)

    def fill_inverse(b):
        first = pl.multiple_of(b * 64, 64)
        for out, size, tiles in ((t1, 1280, 10), (t2, 640, 5), (t3, 320, 3)):

            def store(a, value, out=out):
                out[pl.ds(first, 64), 128 * a : 128 * a + 128] = value.astype(BF16)

            fill_table(cols, 1536 + first, 64, size, 1.0 / math.sqrt(size), tiles, store)

    each(0, 12, fill_inverse)
    for copy in tables:
        copy.start()

    def take_group(g):
        y_wait(g)
        fold_fields(2 * g, x, folded, wide)
        fold_fields(2 * g + 1, x, folded, wide)

        @pl.when(g == 0)
        def _():
            relay(2)

        @pl.when(g == 2)
        def _():
            relay(3)
            start_last()

    each(0, 4, take_group)
    for copy in loads:
        copy.wait()
    for k in range(1, NFLD):
        extra_copy(k).wait()
    for k in range(NFLD):
        back = lax.dot_general(
            columns[k, :, 0:rows], unit, (((0,), (0,)), ((), ())), preferred_element_type=F32
        )
        extra[rows * k : rows * k + rows] = back.astype(BF16)

    parts = ((early, early_in), (late, late_in))

    def block_copy(part, k):
        return to_lat(
            parts[part][0].at[lat_peer(k)],
            parts[part][1].at[lat],
            block_send.at[part],
            block_recv.at[part],
            k,
        )

    def whole(q):
        far(q, lax.rem(q, 2)).wait_recv()

    def pair(q):
        p = assign_s[PAIR * lat + q]
        legendre_pair(q, p, limits, wide, main, extra, synths, joined, levels)

    def send_part(part):
        turn_levels(part, levels, turned, pickers, parts[part][0])
        parts[part][1][lat] = parts[part][0][lat]
        each(1, NLAT, lambda k: block_copy(part, k).start())

    def take_part(part):
        count = pl.ds(0, NLAT - 1)
        both = to_lat(
            parts[part][0].at[count], parts[part][1].at[count], block_send.at[part],
            block_recv.at[part], 1,
        )
        both.wait_send()
        both.wait_recv()

    def early_pair(q):
        whole(q)
        pair(q)

    each(0, EARLY, early_pair)
    send_part(0)
    near_last(8, 0).wait_recv()
    far(8, 0).start()
    near_last(9, 1).wait_recv()
    far(9, 1).start()
    near_last(8, 1).wait_recv()
    near_last(9, 0).wait_recv()
    for q in range(EARLY, PAIR):
        whole(q)
    for q in range(EARLY, PAIR):
        pair(q)
    send_part(1)

    def field(f):
        part = strided(joined, 0, 6, f, 2 * PAIR, FLD)
        spec[f] = part[:, 0:641].reshape(PAIR, 2, 641).astype(BF16)

    each(0, FLD, field)
    spec_copy = pltpu.make_async_copy(spec, spec_out, store_sem.at[4])
    spec_copy.start()

    first_two = main.at[:, pl.ds(0, 2 * rows)]
    to_fld(first_two, near_send, near_recv.at[0, 0], 1).wait_send()
    to_fld(main.at[:, pl.ds(0, rows)], far_send, far_recv.at[0], 1).wait_send()
    take_part(0)
    spread_early(early_in, wide)
    for k, (table_k, p) in enumerate(((t1, p1), (t2, p2), (t3, p3))):
        first, count = LEVEL_ROWS[k]
        tiles = [wide[tile, first : first + count, :] for tile in range(4)]
        lhs = jnp.concatenate(tiles, axis=1).astype(BF16)
        p[...] = jnp.dot(lhs, table_k[0:DEEP], preferred_element_type=F32)
    products = [
        pltpu.make_async_copy(a, b, store_sem.at[5 + k])
        for k, (a, b) in enumerate(((p1, p1_out), (p2, p2_out), (p3, p3_out)))
    ]
    for copy in products:
        copy.start()
    take_part(1)
    spread_late(late_in, wide)
    done = 0
    for first, count in LEVEL_ROWS:
        rows_v[done : done + count] = wide[4, first : first + count, :].astype(BF16)
        done += count
    rows_copy = pltpu.make_async_copy(rows_v, rows_out, store_sem.at[3])
    rows_copy.start()
    for copy in products:
        copy.wait()
    for copy in tables:
        copy.wait()
    spec_copy.wait()
    rows_copy.wait()


def main_step(assign, limits, fields, legendre_t, synths):
    hbm = pl.BlockSpec(memory_space=pltpu.HBM)
    vmem = pl.BlockSpec(memory_space=pltpu.VMEM)
    smem = pl.BlockSpec(memory_space=pltpu.SMEM)
    dma = pltpu.SemaphoreType.DMA
    rows = legendre_t.shape[1]
    synths = [s.reshape(PAIR, 2, m // 2, m) for s, m in zip(synths, LEVELS)]
    wides = (1280, 640, 384)
    return pl.pallas_call(
        main_kernel,
        in_specs=[smem, smem, vmem] + [hbm] * 5,
        out_specs=[hbm] * 8,
        out_shape=[
            jax.ShapeDtypeStruct((FLD, PAIR, 2, 641), BF16),
            jax.ShapeDtypeStruct((FLD * sum(SENT), 128), BF16),
            *[jax.ShapeDtypeStruct((n, w), F32) for (_, n), w in zip(LEVEL_ROWS, wides)],
            *[jax.ShapeDtypeStruct((128, w), BF16) for w in wides],
        ],
        scratch_shapes=[
            pltpu.VMEM((PAIR, rows, 641), BF16),
            pltpu.VMEM((PAIR, NFLD * rows, 640), BF16),
            pltpu.VMEM((NFLD * rows, 128), BF16),
            pltpu.VMEM((NFLD, 16, 256), BF16),
            pltpu.VMEM((1536, LON // 2), BF16),
            pltpu.VMEM((FLD, ROWS, LON), BF16),
            pltpu.VMEM((256, LON // 2), BF16),
            pltpu.VMEM((NLAT, 40, 1024), BF16),
            pltpu.VMEM((NLAT, 40, 1024), BF16),
            pltpu.VMEM((2, NLAT // 2, 40, 128), F32),
            pltpu.VMEM((10, 40 * FLD, 128), F32),
            pltpu.VMEM((6, 48 * PAIR, 128), F32),
            pltpu.VMEM((12, 48 * PAIR, 128), F32),
            pltpu.VMEM((512, 768), F32),
            pltpu.VMEM((FLD, PAIR, 2, 641), BF16),
            pltpu.VMEM((NLAT, 40, 384), BF16),
            pltpu.VMEM((NLAT, 40, 128), BF16),
            pltpu.VMEM((NLAT, 40, 384), BF16),
            pltpu.VMEM((NLAT, 40, 128), BF16),
            pltpu.VMEM((FLD * sum(SENT), 128), BF16),
            pltpu.VMEM((2, 640, 768), BF16),
            pltpu.VMEM((2304, 8), F32),
            pltpu.VMEM((256, 256), BF16),
            *[pltpu.VMEM(s.shape, BF16) for s in synths],
            *[pltpu.VMEM((768, w), BF16) for w in wides],
            *[pltpu.VMEM((n, w), F32) for (_, n), w in zip(LEVEL_ROWS, wides)],
            dma((PAIR,)), dma((4,)), dma((3,)), dma((8,)),
            dma((4,)), dma((4,)), dma, dma((2, 6)), dma, dma((PAIR,)),
            dma((NFLD - 1,)), dma((NFLD - 1,)), dma((2,)), dma((2,)),
        ],
        compiler_params=pltpu.CompilerParams(
            collective_id=0, has_side_effects=True, vmem_limit_bytes=64 * 1000 * 1000
        ),
    )(assign, limits, assign, fields, legendre_t, *synths)


CHUNKS = ((0, 0, 6), (0, 6, 6), (0, 12, 8), (1, 0, 10), (2, 0, 5))


def inverse_kernel(
    rows_in, spec_in, p1_in, p2_in, p3_in, t1_in, t2_in, t3_in,
    spec_out, o1_out, o2_out, o3_out,
    rows, spec, p1, p2, p3, t1, t2, t3, o1, o2, o3, in_sem, part_sem, out_sem,
):
    sums, outs = (p1, p2, p3), (o1, o2, o3)
    sources, results, tables = (p1_in, p2_in, p3_in), (o1_out, o2_out, o3_out), (t1, t2, t3)
    small = [
        pltpu.make_async_copy(a, b, in_sem.at[k])
        for k, (a, b) in enumerate(
            ((rows_in, rows), (t1_in, t1), (t2_in, t2), (t3_in, t3), (spec_in, spec))
        )
    ]
    loads, stores = [], []
    for k, (level, first, count) in enumerate(CHUNKS):
        part = pl.ds(FLD * first, FLD * count)
        loads.append(
            pltpu.make_async_copy(
                sources[level].at[part], sums[level].at[part], part_sem.at[k]
            )
        )
        part = pl.ds(first, count)
        stores.append(
            pltpu.make_async_copy(outs[level].at[part], results[level].at[part], out_sem.at[k])
        )
    for copy in small[0:2] + loads[0:3] + small[2:4] + loads[3:5] + small[4:5]:
        copy.start()
    small[0].wait()
    spec_store = pltpu.make_async_copy(spec, spec_out, out_sem.at[len(CHUNKS)])
    begin = (0, 20, 30)
    for k, (level, first, count) in enumerate(CHUNKS):
        if first == 0:
            small[1 + level].wait()
        loads[k].wait()
        start = FLD * (begin[level] + first)
        lhs = rows[start : start + FLD * count]
        z = jnp.dot(lhs, tables[level][...], preferred_element_type=F32)
        z = z + sums[level][FLD * first : FLD * (first + count)]
        size = outs[level].shape[2]
        outs[level][first : first + count] = z[:, 0:size].reshape(count, FLD, size)
        stores[k].start()
    small[4].wait()
    spec_store.start()
    for copy in stores:
        copy.wait()
    spec_store.wait()


def inverse_step(rows, spectrum, products, tables):
    shapes = [(n, FLD, 4 * m) for n, m in zip(SENT, LEVELS)]
    hbm = pl.BlockSpec(memory_space=pltpu.HBM)
    dma = pltpu.SemaphoreType.DMA
    inputs = (rows, spectrum, *products, *tables)
    return pl.pallas_call(
        inverse_kernel,
        in_specs=[hbm] * 8,
        out_specs=[hbm] * 4,
        out_shape=[jax.ShapeDtypeStruct(spectrum.shape, spectrum.dtype)]
        + [jax.ShapeDtypeStruct(s, F32) for s in shapes],
        scratch_shapes=[pltpu.VMEM(a.shape, a.dtype) for a in inputs]
        + [pltpu.VMEM(s, F32) for s in shapes]
        + [dma((5,)), dma((len(CHUNKS),)), dma((len(CHUNKS) + 1,))],
    )(*inputs)


def on_device(grid_fields, assign, limits, legendre, synth_one, synth_two, synth_three):
    spectrum, rows, *rest = main_step(
        assign,
        limits,
        grid_fields,
        jnp.transpose(legendre, (0, 2, 1)),
        (synth_one, synth_two, synth_three),
    )
    spectrum, *grids = inverse_step(rows, spectrum, rest[0:3], rest[3:6])
    return (
        jnp.transpose(spectrum, (0, 2, 1, 3)),
        *[jnp.transpose(g, (1, 0, 2)) for g in grids],
    )


def solution(mesh):
    return jax.shard_map(
        on_device,
        mesh=mesh,
        in_specs=(
            P("fld", "lat", None),
            P(),
            P(),
            P("lat", None, "fld"),
            P("lat", None, None),
            P("lat", None, None),
            P("lat", None, None),
        ),
        out_specs=(
            P("fld", None, "lat", None),
            P("fld", "lat", None),
            P("fld", "lat", None),
            P("fld", "lat", None),
        ),
        check_vma=False,
    )
```
